8 devices in a mesh: dp: 1 (over z), ep: 8 (over y, x, core).
Axes of the slice: x: 2, y: 2, z: 1, core: 2. Of those that a mesh axis runs over, the one named last changes fastest.
Arguments:
- x_in: bfloat16 [1024, 2048], P(('dp', 'ep'))
- expert_ids: int32 [1024, 6], P(('dp', 'ep'))
- norm_weight: bfloat16 [2048], replicated
- router_w: bfloat16 [2048, 64], replicated
- router_b: bfloat16 [64], replicated
- w_gate_up: bfloat16 [64, 2048, 2816], P('ep')
- b_gate_up: bfloat16 [64, 2816], P('ep')
- w_down: bfloat16 [64, 1408, 2048], P('ep')
- b_down: bfloat16 [64, 2048], P('ep')
Outputs:
- output: bfloat16 [1024, 2048], P(('dp', 'ep'))
All inputs are finite; a program needn't handle non-finite values.
Results may differ from the reference program's by a relative error of at most 0.00655539.
Values are sent between devices in bfloat16 or wider.
A program may use at most 1 GiB of HBM per device.

```python
import jax
import jax.numpy as jnp
from jax import lax

D_MODEL = 2048
D_FF = 1408
EXPERTS = 64
TOP_K = 6
TOK_DEV = 128
GROUP_SIZE = 8

TOKENS = TOK_DEV * GROUP_SIZE
CAPACITY = 4 * TOP_K * TOK_DEV // EXPERTS
HOT_COUNT = EXPERTS // 8
EPSILON = 1e-5
LIMIT = 7.0
ALPHA = 1.702


def draw_routes(key):
    key_hot, key_src = jax.random.split(key)
    expert_order = jax.random.permutation(key_hot, EXPERTS)
    cold_total = TOP_K * TOK_DEV - HOT_COUNT * CAPACITY
    cold_count = EXPERTS - HOT_COUNT
    position = jnp.arange(EXPERTS)
    extra = (position - HOT_COUNT < cold_total % cold_count).astype(jnp.int32)
    counts = jnp.where(position < HOT_COUNT, CAPACITY, cold_total // cold_count + extra)
    ends = jnp.cumsum(counts)
    slot_rank = jnp.sum(jnp.arange(TOP_K * TOK_DEV)[:, None] >= ends[None, :], axis=1)

    def one_source(src_key):
        key_cold, key_tok = jax.random.split(src_key)
        cold = jax.random.permutation(key_cold, expert_order[HOT_COUNT:])
        order = jnp.concatenate([expert_order[:HOT_COUNT], cold])
        table = order[slot_rank].reshape(TOP_K, TOK_DEV).T
        return table[jax.random.permutation(key_tok, TOK_DEV)]

    tables = jax.vmap(one_source)(jax.random.split(key_src, GROUP_SIZE))
    return tables.reshape(TOKENS, TOP_K).astype(jnp.int32)


def stacked_normal(key, shape, scale):
    def one_expert(expert_key):
        return (jax.random.normal(expert_key, shape, jnp.float32) * scale).astype(jnp.bfloat16)
    return lax.map(one_expert, jax.random.split(key, EXPERTS))


def setup_inputs(seed: int = 0, part: int = 0) -> dict:
    shared = jax.random.split(jax.random.key(seed), 7)
    own = jax.random.split(jax.random.fold_in(jax.random.key(seed + 1), part), 2)
    x_in = jax.random.normal(own[0], (TOKENS, D_MODEL), jnp.float32).astype(jnp.bfloat16)
    expert_ids = draw_routes(own[1])
    norm_weight = (1.0 + 0.3 * jax.random.normal(shared[0], (D_MODEL,), jnp.float32)).astype(jnp.bfloat16)
    router_w = (jax.random.normal(shared[1], (D_MODEL, EXPERTS), jnp.float32) * D_MODEL ** -0.5).astype(jnp.bfloat16)
    router_b = (0.7 * jax.random.normal(shared[2], (EXPERTS,), jnp.float32)).astype(jnp.bfloat16)
    w_gate_up = stacked_normal(shared[3], (D_MODEL, 2 * D_FF), 5.0 * D_MODEL ** -0.5)
    b_gate_up = jax.random.normal(shared[4], (EXPERTS, 2 * D_FF), jnp.float32).astype(jnp.bfloat16)
    w_down = stacked_normal(shared[5], (D_FF, D_MODEL), 0.125 * D_FF ** -0.5)
    b_down = (0.5 * jax.random.normal(shared[6], (EXPERTS, D_MODEL), jnp.float32)).astype(jnp.bfloat16)
    return dict(x_in=x_in, expert_ids=expert_ids, norm_weight=norm_weight, router_w=router_w, router_b=router_b, w_gate_up=w_gate_up, b_gate_up=b_gate_up, w_down=w_down, b_down=b_down)


def clamped_glu(gate_up):
    gate = jnp.minimum(gate_up[..., 0::2].astype(jnp.float32), LIMIT)
    linear = jnp.clip(gate_up[..., 1::2].astype(jnp.float32), -LIMIT, LIMIT)
    return (gate * jax.nn.sigmoid(ALPHA * gate) * (linear + 1.0)).astype(jnp.bfloat16)


def reference(x_in, expert_ids, norm_weight, router_w, router_b, w_gate_up, b_gate_up, w_down, b_down):
    x_float = x_in.astype(jnp.float32)
    inv_rms = lax.rsqrt(jnp.mean(x_float * x_float, axis=-1, keepdims=True) + EPSILON)
    hidden = (x_float * inv_rms * norm_weight.astype(jnp.float32)).astype(jnp.bfloat16)
    logits = jnp.dot(hidden, router_w, preferred_element_type=jnp.float32) + router_b.astype(jnp.float32)
    gates = jax.nn.softmax(jnp.take_along_axis(logits, expert_ids, axis=1), axis=-1)
    flat_ids = expert_ids.reshape(-1)
    flat_gates = gates.reshape(-1)
    max_rows = GROUP_SIZE * CAPACITY

    def one_expert(combined, weights):
        expert, gate_up_w, gate_up_b, down_w, down_b = weights
        chosen = flat_ids == expert
        picks = jnp.nonzero(chosen, size=max_rows, fill_value=0)[0]
        valid = jnp.arange(max_rows) < jnp.sum(chosen)
        row_token = picks // TOP_K
        rows = hidden[row_token]
        gate_up = (jnp.dot(rows, gate_up_w, preferred_element_type=jnp.float32) + gate_up_b.astype(jnp.float32)).astype(jnp.bfloat16)
        glu_out = clamped_glu(gate_up)
        expert_out = (jnp.dot(glu_out, down_w, preferred_element_type=jnp.float32) + down_b.astype(jnp.float32)).astype(jnp.bfloat16)
        scale = jnp.where(valid, flat_gates[picks], 0.0)
        combined = combined.at[row_token].add(scale[:, None] * expert_out.astype(jnp.float32))
        return combined, None

    start_sum = jnp.zeros((TOKENS, D_MODEL), jnp.float32)
    combined, _ = lax.scan(one_expert, start_sum, (jnp.arange(EXPERTS, dtype=jnp.int32), w_gate_up, b_gate_up, w_down, b_down))
    return (x_float + combined).astype(jnp.bfloat16)
```

```python
import functools

import jax
import jax.numpy as jnp
from jax import lax
from jax.experimental import pallas as pl
from jax.experimental.pallas import tpu as pltpu
from jax.sharding import PartitionSpec as P

CAPACITY_FACTOR = 4
EPSILON = 1e-5
LIMIT = 7.0
ALPHA = 1.702
LOWEST = -3.3895313892515355e38
BLK = 16
CHUNK = 128
COLS = 256
MESH = pl.DeviceIdType.MESH
F32 = jnp.float32
BF16 = jnp.bfloat16
VMEM_LIMIT = 62 * 1024 * 1024


def flip(me, role):
    core = lax.rem(lax.rem(me, 2) + lax.rem(role, 2), 2)
    x = lax.rem(lax.rem(lax.div(me, 2), 2) + lax.rem(lax.div(role, 2), 2), 2)
    y = lax.rem(lax.div(me, 4) + lax.div(role, 4), 2)
    return y * 4 + x * 2 + core


def remote(src, dst, send, recv, device):
    return pltpu.make_async_remote_copy(src_ref=src, dst_ref=dst, send_sem=send, recv_sem=recv, device_id={'ep': device}, device_id_type=MESH)


def dispatch_kernel(top_k, local_exp, cap, x_hbm, ids_hbm, g_ref, wr_ref, br_ref, xs_hbm, pm_hbm, cnt_ref,
                    xb, idb, hb, wrp, brp, tri, oh, pt, probs, mask, stage, pstage,
                    lsem, osem, psem, ssem, rsem, isend, irecv):
    tok, d_model = x_hbm.shape
    experts = wr_ref.shape[1]
    half = tok // 2
    me = lax.axis_index('ep')
    load_x = pltpu.make_async_copy(x_hbm, xb.at[0], lsem.at[0])
    load_ids = pltpu.make_async_copy(ids_hbm, idb.at[0], lsem.at[1])
    load_x.start()
    load_ids.start()
    barrier = pltpu.get_barrier_semaphore()
    for r in range(1, 8):
        pl.semaphore_signal(barrier, inc=1, device_id={'ep': flip(me, r)}, device_id_type=MESH)
    load_x.wait()
    load_ids.wait()
    pl.semaphore_wait(barrier, 7)

    def piece(src_role, h, dst_role, to_role, k):
        rows = pl.ds(h * half, half)
        return remote(xb.at[src_role, rows], xb.at[dst_role, rows], ssem.at[k], rsem.at[dst_role, h], flip(me, to_role))

    def landed(role, h):
        piece(role, h, role, 1, 0).wait_recv()

    sends = [(0, 0, 2, 2), (0, 1, 4, 4), (0, 0, 1, 1), (0, 1, 1, 1), (0, 1, 2, 2), (0, 0, 4, 4)]
    relays = [(2, 0, 6, 4), (2, 0, 3, 1), (4, 1, 6, 2), (4, 1, 5, 1), (2, 1, 3, 1), (4, 0, 5, 1)]
    last = [(6, 0, 7, 1), (6, 1, 7, 1)]
    everything = sends + relays + last
    ids_out = [remote(idb.at[0], idb.at[r], isend.at[r], irecv.at[r], flip(me, r)) for r in range(1, 8)]
    for c in ids_out:
        c.start()

    def go(k):
        piece(*everything[k], k).start()

    for k in range(6):
        go(k)

    wrp[...] = jnp.zeros_like(wrp)
    wrp[:, :experts] = wr_ref[...]
    brp[...] = jnp.zeros_like(brp)
    brp[0:1, :experts] = br_ref[...].astype(F32)
    tri[...] = (lax.broadcasted_iota(jnp.int32, (tok, tok), 0) < lax.broadcasted_iota(jnp.int32, (tok, tok), 1)).astype(F32).astype(BF16)
    cnt_ref[...] = jnp.zeros_like(cnt_ref)

    def step(i, carry):
        @pl.when(i == 1)
        def _():
            landed(1, 0)
            landed(1, 1)

        @pl.when(i == 2)
        def _():
            landed(2, 0)
            go(6)
            go(7)
            landed(4, 1)
            go(8)
            go(9)
            landed(2, 1)
            go(10)
            landed(4, 0)
            go(11)

        @pl.when(i == 3)
        def _():
            landed(3, 0)
            landed(3, 1)

        @pl.when(i == 5)
        def _():
            landed(5, 0)
            landed(5, 1)

        @pl.when(i == 6)
        def _():
            landed(6, 0)
            go(12)
            landed(6, 1)
            go(13)

        @pl.when(i == 7)
        def _():
            landed(7, 0)
            landed(7, 1)

        @pl.when(i >= 1)
        def _():
            remote(idb.at[i], idb.at[i], isend.at[0], irecv.at[i], flip(me, 1)).wait_recv()

        src = flip(me, i)
        slot = lax.rem(i, 2)
        out_x = pltpu.make_async_copy(stage.at[slot], xs_hbm.at[:, src], osem.at[slot])
        out_p = pltpu.make_async_copy(pstage.at[slot], pm_hbm.at[src], psem.at[slot])

        def norm(j, c):
            rows = pl.ds(pl.multiple_of(j * BLK, BLK), BLK)
            xf = xb[i, rows, :].astype(F32)
            inv = lax.rsqrt(jnp.mean(xf * xf, axis=-1, keepdims=True) + EPSILON)
            hb[rows, :] = (xf * inv * g_ref[...].astype(F32)).astype(BF16)
            return c

        lax.fori_loop(0, tok // BLK, norm, 0)
        logits = jnp.dot(hb[...], wrp[...], preferred_element_type=F32) + brp[0:1, :]
        logits = jnp.transpose(logits)[:experts]
        ids = idb[i]
        expert_no = lax.broadcasted_iota(jnp.int32, (experts, tok), 0)
        chosen = jnp.zeros((experts, tok), F32)
        for k in range(top_k):
            chosen = jnp.where(expert_no == ids[k:k + 1, :], 1.0, chosen)
        picked = jnp.where(chosen > 0, logits, -jnp.inf)
        ex = jnp.exp(picked - jnp.max(picked, axis=0, keepdims=True))
        probs[...] = ex / jnp.sum(ex, axis=0, keepdims=True)
        mask[...] = chosen
        mine = pl.ds(pl.multiple_of(me * local_exp, local_exp), local_exp)
        p_loc = probs[mine, :]
        m_loc = mask[mine, :]
        rank = jnp.dot(m_loc.astype(BF16), tri[...], preferred_element_type=F32)
        count = jnp.sum(m_loc, axis=1, keepdims=True)
        lane = lax.broadcasted_iota(jnp.int32, cnt_ref.shape, 1)
        cnt_ref[...] = jnp.where(lane == src, count.astype(jnp.int32), cnt_ref[...])
        rank = jnp.where(m_loc > 0, rank, -1.0)
        number = lax.broadcasted_iota(jnp.int32, (cap, tok), 0).astype(F32)

        @pl.when(i >= 2)
        def _():
            out_x.wait()
            out_p.wait()

        for e in range(local_exp):
            hit = rank[e:e + 1, :] == number
            oh[e * cap:(e + 1) * cap, :] = jnp.where(hit, 1.0, 0.0).astype(BF16)
            pt[e * cap:(e + 1) * cap, :] = jnp.where(hit, p_loc[e:e + 1, :], 0.0)
        for b in range(local_exp * cap // tok):
            p = jnp.transpose(pt[b * tok:(b + 1) * tok, :])
            for part in range(3):
                low = p.astype(BF16)
                pstage[slot, part * tok:(part + 1) * tok, b * tok:(b + 1) * tok] = low
                p = p - low.astype(F32)
        for n in range(0, d_model, 512):
            rows = jnp.dot(oh[...], hb[:, n:n + 512], preferred_element_type=F32).astype(BF16)
            for e in range(local_exp):
                stage[slot, e, :, n:n + 512] = rows[e * cap:(e + 1) * cap, :]
        out_x.start()
        out_p.start()
        return carry

    lax.fori_loop(0, 8, step, 0)
    for slot in range(2):
        pltpu.make_async_copy(stage.at[slot], xs_hbm.at[:, me], osem.at[slot]).wait()
        pltpu.make_async_copy(pstage.at[slot], pm_hbm.at[me], psem.at[slot]).wait()
    for c in ids_out:
        c.wait_send()
    for k in range(len(everything)):
        piece(*everything[k], k).wait_send()


def gate_up_kernel(cnt_ref, xs_hbm, wgu_hbm, bgu_ref, z_hbm, wb, xbuf, xc, zc, zb, bias, perm, blk, wsem, xsem, zsem):
    local_exp, n_src, cap, d_model = xs_hbm.shape
    width = wgu_hbm.shape[2]
    rows_all = n_src * cap
    per_src = cap // BLK
    n_blk = rows_all // BLK
    n_slot = wb.shape[0]

    def load_w(e):
        slot = lax.rem(e, n_slot)
        return pltpu.make_async_copy(wgu_hbm.at[e], wb.at[slot], wsem.at[slot])

    def load_x(e):
        slot = lax.rem(e, 2)
        return pltpu.make_async_copy(xs_hbm.at[e], xbuf.at[slot], xsem.at[slot])

    def save_z(e):
        slot = lax.rem(e, 2)
        return pltpu.make_async_copy(zb.at[slot, pl.ds(0, rows_all)], z_hbm.at[e], zsem.at[slot])

    for e in range(2):
        load_x(e).start()
    for e in range(n_slot):
        load_w(e).start()
    bias[...] = bgu_ref[...].astype(F32)
    row = lax.broadcasted_iota(jnp.int32, perm.shape, 0)
    col = lax.broadcasted_iota(jnp.int32, perm.shape, 1)
    source = jnp.where(col < 128, 2 * col, 2 * col - 255)
    perm[...] = jnp.where(row == source, 1.0, 0.0).astype(BF16)

    def expert(e, carry):
        slot = lax.rem(e, n_slot)
        pair = lax.rem(e, 2)

        def listed(s, n):
            k = lax.div(cnt_ref[e, s] + (BLK - 1), BLK)
            for b in range(per_src):
                @pl.when(b < k)
                def _():
                    blk[n + b] = s * per_src + b
            return n + k

        total = lax.fori_loop(0, n_src, listed, 0)
        for j in range(CHUNK // BLK):
            blk[total + j] = n_blk

        @pl.when(e >= 2)
        def _():
            save_z(e - 2).wait()

        zb[pair] = jnp.zeros(zb.shape[1:], BF16)
        load_x(e).wait()
        load_w(e).wait()

        def chunk(c, carry):
            for j in range(CHUNK // BLK):
                b = jnp.minimum(blk[c * (CHUNK // BLK) + j], n_blk - 1)
                s = lax.div(b, per_src)
                first = pl.multiple_of(lax.rem(b, per_src) * BLK, BLK)
                xc[j * BLK:(j + 1) * BLK, :] = xbuf[pair, s, pl.ds(first, BLK), :]
            for n in range(0, width, 512):
                w = min(512, width - n)
                u = jnp.dot(xc[...], wb[slot, :, n:n + w], preferred_element_type=F32) + bias[pl.ds(e, 1), n:n + w]
                u = jnp.minimum(jnp.maximum(u, LOWEST), LIMIT).astype(BF16)
                for m in range(0, w, 256):
                    v = jnp.dot(u[:, m:m + 256], perm[...], preferred_element_type=F32)
                    gate = v[:, :128]
                    linear = jnp.maximum(v[:, 128:], -LIMIT)
                    z = gate * lax.logistic(ALPHA * gate) * (linear + 1.0)
                    zc[:, (n + m) // 2:(n + m) // 2 + 128] = z.astype(BF16)
            for j in range(CHUNK // BLK):
                b = blk[c * (CHUNK // BLK) + j]
                zb[pair, pl.ds(pl.multiple_of(b * BLK, BLK), BLK), :] = zc[j * BLK:(j + 1) * BLK, :]
            return carry

        lax.fori_loop(0, lax.div(total + (CHUNK // BLK - 1), CHUNK // BLK), chunk, 0)
        save_z(e).start()

        @pl.when(e + n_slot < local_exp)
        def _():
            load_w(e + n_slot).start()

        @pl.when(e + 2 < local_exp)
        def _():
            load_x(e + 2).start()
        return carry

    lax.fori_loop(0, local_exp, expert, 0)
    for e in range(local_exp - 2, local_exp):
        save_z(e).wait()


def combine_kernel(z_hbm, pm_hbm, wd_hbm, bd_ref, x_ref, out_ref,
                   zb, pm, wb, bias, yb, part, in0, in1, in2,
                   zsem, psem, wsem, s0, s1, s2, r0, r1, r2):
    local_exp, rows_all, d_ff = z_hbm.shape
    n_src = 8
    cap = rows_all // n_src
    tok, d_model = x_ref.shape
    n_col = d_model // COLS
    me = lax.axis_index('ep')
    barrier = pltpu.get_barrier_semaphore()
    for r in (1, 2, 4):
        pl.semaphore_signal(barrier, inc=1, device_id={'ep': flip(me, r)}, device_id_type=MESH)

    def load_w(c):
        slot = lax.rem(c, 2)
        cols = pl.ds(pl.multiple_of(c * COLS, COLS), COLS)
        return pltpu.make_async_copy(wd_hbm.at[:, :, cols], wb.at[slot], wsem.at[slot])

    load_w(0).start()
    zload = pltpu.make_async_copy(z_hbm, zb, zsem)
    pload = pltpu.make_async_copy(pm_hbm, pm, psem)
    zload.start()
    pload.start()
    bias[...] = bd_ref[...].astype(F32)

    def order(c):
        parity = lax.rem(c, 2)
        first = 2 + 2 * parity
        return first, 6 - first

    def to_mate(c):
        return remote(part.at[c, 1], in0.at[c], s0.at[c], r0.at[c], flip(me, 1))

    def to_first(c):
        return remote(part.at[c, 0, pl.ds(2, 2)], in1.at[c], s1.at[c], r1.at[c], flip(me, order(c)[0]))

    def to_second(c):
        return remote(part.at[c, 0, 1], in2.at[c], s2.at[c], r2.at[c], flip(me, order(c)[1]))

    def merge_mate(c):
        to_mate(c).wait_recv()
        for j in (2, 3, 0, 1):
            part[c, 0, j] = part[c, 0, j] + in0[c, j]
        to_first(c).start()

    def merge_first(c):
        to_first(c).wait_recv()
        for j in (1, 0):
            part[c, 0, j] = part[c, 0, j] + in1[c, j]
        to_second(c).start()

    def finish(c):
        to_second(c).wait_recv()
        cols = pl.ds(pl.multiple_of(c * COLS, COLS), COLS)
        out_ref[:, cols] = (x_ref[:, cols].astype(F32) + (part[c, 0, 0] + in2[c])).astype(BF16)

    def step(c, carry):
        slot = lax.rem(c, 2)
        cols = pl.ds(pl.multiple_of(c * COLS, COLS), COLS)

        @pl.when(c + 1 < n_col)
        def _():
            load_w(c + 1).start()

        @pl.when(c == 0)
        def _():
            zload.wait()
            pload.wait()

        load_w(c).wait()
        for e in range(local_exp):
            y = jnp.dot(zb[e], wb[slot, e], preferred_element_type=F32) + bias[e:e + 1, cols]
            y = y.astype(BF16)
            for s in range(n_src):
                yb[s, e * cap:(e + 1) * cap, :] = y[s * cap:(s + 1) * cap, :]
        first, second = order(c)
        for core in (1, 0):
            for j, base in enumerate((0, second, first, 6)):
                src = flip(me, base + core)
                sums = jnp.dot(pm[src], yb[src], preferred_element_type=F32)
                part[c, core, j] = (sums[2 * tok:] + sums[tok:2 * tok]) + sums[:tok]

        @pl.when(c == 0)
        def _():
            pl.semaphore_wait(barrier, 3)

        to_mate(c).start()

        @pl.when(c >= 1)
        def _():
            merge_mate(c - 1)

        @pl.when(c >= 3)
        def _():
            merge_first(c - 3)

        @pl.when(c >= 5)
        def _():
            finish(c - 5)
        return carry

    lax.fori_loop(0, n_col, step, 0)
    merge_mate(n_col - 1)
    for c in range(n_col - 3, n_col):
        merge_first(c)
    for c in range(n_col - 5, n_col):
        finish(c)
    for c in range(n_col):
        to_mate(c).wait_send()
        to_first(c).wait_send()
        to_second(c).wait_send()


def solution(mesh):
    n_group = mesh.shape['ep']
    assert n_group == 8
    rows_spec = P(('dp', 'ep'), None)

    def local_block(x_in, expert_ids, norm_weight, router_w, router_b, w_gate_up, b_gate_up, w_down, b_down):
        tok, d_model = x_in.shape
        top_k = expert_ids.shape[1]
        local_exp, _, width = w_gate_up.shape
        d_ff = w_down.shape[1]
        experts = local_exp * n_group
        cap = CAPACITY_FACTOR * top_k * tok // experts
        rows_all = n_group * cap
        ids_t = jnp.pad(expert_ids.T, ((0, 8 - top_k), (0, 0)), constant_values=-1)
        hbm = pl.BlockSpec(memory_space=pl.ANY)
        vmem = pl.BlockSpec(memory_space=pltpu.VMEM)
        smem = pl.BlockSpec(memory_space=pltpu.SMEM)
        dma = pltpu.SemaphoreType.DMA
        xs, pm, counts = pl.pallas_call(
            functools.partial(dispatch_kernel, top_k, local_exp, cap),
            out_shape=(jax.ShapeDtypeStruct((local_exp, n_group, cap, d_model), BF16),
                       jax.ShapeDtypeStruct((n_group, 3 * tok, local_exp * cap), BF16),
                       jax.ShapeDtypeStruct((local_exp, 128), jnp.int32)),
            in_specs=[hbm, hbm, vmem, vmem, vmem],
            out_specs=(hbm, hbm, vmem),
            scratch_shapes=[
                pltpu.VMEM((8, tok, d_model), BF16), pltpu.VMEM((8, 8, tok), jnp.int32), pltpu.VMEM((tok, d_model), BF16),
                pltpu.VMEM((d_model, 128), BF16), pltpu.VMEM((8, 128), F32), pltpu.VMEM((tok, tok), BF16),
                pltpu.VMEM((local_exp * cap, tok), BF16), pltpu.VMEM((local_exp * cap, tok), F32),
                pltpu.VMEM((experts, tok), F32), pltpu.VMEM((experts, tok), F32),
                pltpu.VMEM((2, local_exp, cap, d_model), BF16), pltpu.VMEM((2, 3 * tok, local_exp * cap), BF16),
                dma((2,)), dma((2,)), dma((2,)), dma((14,)), dma((8, 2)), dma((8,)), dma((8,))],
            compiler_params=pltpu.CompilerParams(collective_id=0, has_side_effects=True, vmem_limit_bytes=VMEM_LIMIT),
            name='dispatch',
        )(x_in, ids_t, norm_weight.reshape(1, d_model), router_w, router_b.reshape(1, experts))
        z = pl.pallas_call(
            gate_up_kernel,
            out_shape=jax.ShapeDtypeStruct((local_exp, rows_all, d_ff), BF16),
            in_specs=[smem, hbm, hbm, vmem],
            out_specs=hbm,
            scratch_shapes=[
                pltpu.VMEM((3, d_model, width), BF16), pltpu.VMEM((2, n_group, cap, d_model), BF16), pltpu.VMEM((CHUNK, d_model), BF16),
                pltpu.VMEM((CHUNK, d_ff), BF16), pltpu.VMEM((2, rows_all + BLK, d_ff), BF16), pltpu.VMEM((local_exp, width), F32),
                pltpu.VMEM((256, 256), BF16), pltpu.SMEM((rows_all // BLK + CHUNK // BLK,), jnp.int32),
                dma((3,)), dma((2,)), dma((2,))],
            compiler_params=pltpu.CompilerParams(vmem_limit_bytes=VMEM_LIMIT),
            name='gate_up',
        )(counts, xs, w_gate_up, b_gate_up)
        n_col = d_model // COLS
        return pl.pallas_call(
            combine_kernel,
            out_shape=jax.ShapeDtypeStruct((tok, d_model), BF16),
            in_specs=[hbm, hbm, hbm, vmem, vmem],
            out_specs=vmem,
            scratch_shapes=[
                pltpu.VMEM((local_exp, rows_all, d_ff), BF16), pltpu.VMEM((n_group, 3 * tok, local_exp * cap), BF16),
                pltpu.VMEM((2, local_exp, d_ff, COLS), BF16), pltpu.VMEM((local_exp, d_model), F32),
                pltpu.VMEM((n_group, local_exp * cap, COLS), BF16), pltpu.VMEM((n_col, 2, 4, tok, COLS), F32),
                pltpu.VMEM((n_col, 4, tok, COLS), F32), pltpu.VMEM((n_col, 2, tok, COLS), F32), pltpu.VMEM((n_col, tok, COLS), F32),
                dma, dma, dma((2,)), dma((n_col,)), dma((n_col,)), dma((n_col,)), dma((n_col,)), dma((n_col,)), dma((n_col,))],
            compiler_params=pltpu.CompilerParams(collective_id=1, has_side_effects=True, vmem_limit_bytes=VMEM_LIMIT),
            name='combine',
        )(z, pm, w_down, b_down, x_in)

    return jax.shard_map(local_block, mesh=mesh, in_specs=(rows_spec, rows_spec, P(), P(), P(), P('ep', None, None), P('ep', None), P('ep', None, None), P('ep', None)), out_specs=rows_spec, check_vma=False)
```

```python
import functools

import jax
import jax.numpy as jnp
from jax import lax
from jax.experimental import pallas as pl
from jax.experimental.pallas import tpu as pltpu
from jax.sharding import PartitionSpec as P

CAPACITY_FACTOR = 4
EPSILON = 1e-5
LIMIT = 7.0
ALPHA = 1.702
LOWEST = -3.3895313892515355e38
BLK = 16
COLS = 256
MESH = pl.DeviceIdType.MESH
F32 = jnp.float32
BF16 = jnp.bfloat16
MIB = 1024 * 1024
N_RING = 3
NSTEP = 1024


def flip(me, role):
    core = lax.rem(lax.rem(me, 2) + lax.rem(role, 2), 2)
    x = lax.rem(lax.rem(lax.div(me, 2), 2) + lax.rem(lax.div(role, 2), 2), 2)
    y = lax.rem(lax.div(me, 4) + lax.div(role, 4), 2)
    return y * 4 + x * 2 + core


def remote(src, dst, send, recv, device):
    return pltpu.make_async_remote_copy(src_ref=src, dst_ref=dst, send_sem=send, recv_sem=recv, device_id={'ep': device}, device_id_type=MESH)


def dispatch_kernel(top_k, local_exp, cap, x_hbm, ids_hbm, g_hbm, wr_hbm, br_hbm, xs_ref, pm_hbm, cnt_hbm,
                    g_ref, wr_ref, br_ref, cnt_ref, xb, idb, hb, brp, gain, tri, oh, pt, probs, prb, pstage,
                    lsem, psem, ssem, rsem, isend, irecv, gsend, grecv):
    tok, d_model = x_hbm.shape
    experts = wr_ref.shape[0]
    half = tok // 2
    me = lax.axis_index('ep')
    load_x = pltpu.make_async_copy(x_hbm, xb.at[0], lsem.at[0])
    load_ids = pltpu.make_async_copy(ids_hbm, idb.at[0], lsem.at[1])
    load_x.start()
    load_ids.start()
    small = [pltpu.make_async_copy(a, b, lsem.at[k + 2]) for k, (a, b) in enumerate([(g_hbm, g_ref), (wr_hbm, wr_ref), (br_hbm, br_ref)])]
    for c in small:
        c.start()
    barrier = pltpu.get_barrier_semaphore()
    for r in range(1, 8):
        pl.semaphore_signal(barrier, inc=1, device_id={'ep': flip(me, r)}, device_id_type=MESH)
    load_x.wait()
    load_ids.wait()
    pl.semaphore_wait(barrier, 7)

    def piece(src_role, h, dst_role, to_role, k):
        rows = pl.ds(h * half, half)
        return remote(xb.at[src_role, rows], xb.at[dst_role, rows], ssem.at[k], rsem.at[dst_role, h], flip(me, to_role))

    def landed(role, h):
        piece(role, h, role, 1, 0).wait_recv()

    sends = [(0, 0, 2, 2), (0, 1, 4, 4), (0, 0, 1, 1), (0, 1, 1, 1), (0, 1, 2, 2), (0, 0, 4, 4)]
    relays = [(2, 0, 6, 4), (2, 0, 3, 1), (4, 1, 6, 2), (4, 1, 5, 1), (2, 1, 3, 1), (4, 0, 5, 1)]
    last = [(6, 0, 7, 1), (6, 1, 7, 1)]
    everything = sends + relays + last

    def go(k):
        piece(*everything[k], k).start()

    for k in range(6):
        go(k)
    ids_out = [remote(idb.at[0], idb.at[r], isend.at[r], irecv.at[r], flip(me, r)) for r in range(1, 8)]
    for c in ids_out:
        c.start()

    for c in small:
        c.wait()
    brp[...] = jnp.zeros_like(brp)
    brp[0:1, :experts] = br_ref[...].astype(F32)
    bias = jnp.transpose(jnp.broadcast_to(brp[0:1, :], (tok, tok)))[:experts]
    gain[...] = g_ref[...].astype(F32).reshape(gain.shape)
    tri[...] = (lax.broadcasted_iota(jnp.int32, (tok, tok), 0) < lax.broadcasted_iota(jnp.int32, (tok, tok), 1)).astype(F32).astype(BF16)
    cnt_ref[...] = jnp.zeros_like(cnt_ref)

    def normed(i):
        def norm(j, c):
            rows = pl.ds(pl.multiple_of(j * 32, 32), 32)
            xf = xb[i, rows, :].astype(F32)
            inv = lax.rsqrt(jnp.mean(xf * xf, axis=-1, keepdims=True) + EPSILON)
            hb[rows, :] = (xf * inv * gain[...]).astype(BF16)
            return c

        lax.fori_loop(0, tok // 32, norm, 0)

    normed(0)
    logits = lax.dot_general(wr_ref[...], hb[...], (((1,), (1,)), ((), ())), preferred_element_type=F32) + bias
    expert_no = lax.broadcasted_iota(jnp.int32, (experts, tok), 0)
    chosen = jnp.zeros((experts, tok), F32)
    for k in range(top_k):
        chosen = jnp.where(expert_no == idb[0, k:k + 1, :], 1.0, chosen)
    picked = jnp.where(chosen > 0, logits, -jnp.inf)
    ex = jnp.exp(picked - jnp.max(picked, axis=0, keepdims=True))
    probs[...] = ex / jnp.sum(ex, axis=0, keepdims=True)

    def block(device):
        return probs.at[pl.ds(pl.multiple_of(device * local_exp, local_exp), local_exp)]

    gates_out = [remote(block(flip(me, r)), prb.at[r], gsend.at[r], grecv.at[r], flip(me, r)) for r in range(1, 8)]
    for c in gates_out:
        c.start()
    prb[0] = probs[pl.ds(pl.multiple_of(me * local_exp, local_exp), local_exp), :]

    def plan(i, carry):
        @pl.when(i >= 1)
        def _():
            remote(idb.at[i], idb.at[i], isend.at[0], irecv.at[i], flip(me, 1)).wait_recv()
            remote(prb.at[i], prb.at[i], gsend.at[0], grecv.at[i], flip(me, 1)).wait_recv()

        src = flip(me, i)
        slot = lax.rem(i, 2)
        out_p = pltpu.make_async_copy(pstage.at[slot], pm_hbm.at[src], psem.at[slot])
        ids = idb[i]
        number = me * local_exp + lax.broadcasted_iota(jnp.int32, (local_exp, tok), 0)
        held = jnp.zeros((local_exp, tok), F32)
        for k in range(top_k):
            held = jnp.where(number == ids[k:k + 1, :], 1.0, held)
        rank = jnp.dot(held.astype(BF16), tri[...], preferred_element_type=F32)
        count = jnp.sum(held, axis=1, keepdims=True)
        lane = lax.broadcasted_iota(jnp.int32, cnt_ref.shape, 1)
        cnt_ref[...] = jnp.where(lane == src, count.astype(jnp.int32), cnt_ref[...])
        rank = jnp.where(held > 0, rank, -1.0)
        place = lax.broadcasted_iota(jnp.int32, (cap, tok), 0).astype(F32)
        p_loc = prb[i]
        for e in range(local_exp):
            hit = rank[e:e + 1, :] == place
            oh[i, e * cap:(e + 1) * cap, :] = jnp.where(hit, 1.0, 0.0).astype(BF16)
            pt[e * cap:(e + 1) * cap, :] = jnp.where(hit, p_loc[e:e + 1, :], 0.0)

        @pl.when(i >= 2)
        def _():
            out_p.wait()

        for b in range(local_exp * cap // tok):
            p = jnp.transpose(pt[b * tok:(b + 1) * tok, :])
            for part in range(3):
                low = p.astype(BF16)
                pstage[slot, part * tok:(part + 1) * tok, b * tok:(b + 1) * tok] = low
                p = p - low.astype(F32)
        out_p.start()
        return carry

    lax.fori_loop(0, 8, plan, 0)
    save_cnt = pltpu.make_async_copy(cnt_ref, cnt_hbm, lsem.at[0])
    save_cnt.start()

    def gather(i, carry):
        @pl.when(i == 1)
        def _():
            landed(1, 0)
            landed(1, 1)

        @pl.when(i == 2)
        def _():
            landed(2, 0)
            go(6)
            go(7)
            landed(4, 1)
            go(8)
            go(9)
            landed(2, 1)
            go(10)
            landed(4, 0)
            go(11)

        @pl.when(i == 3)
        def _():
            landed(3, 0)
            landed(3, 1)

        @pl.when(i == 5)
        def _():
            landed(5, 0)
            landed(5, 1)

        @pl.when(i == 6)
        def _():
            landed(6, 0)
            go(12)
            landed(6, 1)
            go(13)

        @pl.when(i == 7)
        def _():
            landed(7, 0)
            landed(7, 1)

        normed(i)
        src = flip(me, i)
        for n in range(0, d_model, 512):
            rows = jnp.dot(oh[i], hb[:, n:n + 512], preferred_element_type=F32).astype(BF16)
            for e in range(local_exp):
                xs_ref[e, src, :, n:n + 512] = rows[e * cap:(e + 1) * cap, :]
        return carry

    lax.fori_loop(0, 8, gather, 0)
    save_cnt.wait()
    for slot in range(2):
        pltpu.make_async_copy(pstage.at[slot], pm_hbm.at[me], psem.at[slot]).wait()
    for c in ids_out + gates_out:
        c.wait_send()
    for k in range(len(everything)):
        piece(*everything[k], k).wait_send()


def gate_up_kernel(cnt_hbm, xs_ref, wgu_hbm, bgu_hbm, z_ref, wb, xc, zc, uc, braw, bias, perm, cnt, blk, total, wsem, sem):
    local_exp, n_src, cap, d_model = xs_ref.shape
    width = wgu_hbm.shape[2]
    per_src = cap // BLK
    n_slot = wb.shape[0]

    def load_w(e):
        slot = lax.rem(e, n_slot)
        return pltpu.make_async_copy(wgu_hbm.at[e], wb.at[slot], wsem.at[slot])

    load_cnt = pltpu.make_async_copy(cnt_hbm, cnt, sem.at[0])
    load_bias = pltpu.make_async_copy(bgu_hbm, braw, sem.at[1])
    load_cnt.start()
    load_bias.start()
    for e in range(n_slot):
        load_w(e).start()
    row = lax.broadcasted_iota(jnp.int32, perm.shape, 0)
    col = lax.broadcasted_iota(jnp.int32, perm.shape, 1)
    source = jnp.where(col < 128, 2 * col, 2 * col - 255)
    perm[...] = jnp.where(row == source, 1.0, 0.0).astype(BF16)
    load_cnt.wait()

    def listed(e, carry):
        z_ref[e] = jnp.zeros(z_ref.shape[1:], BF16)
        n = jnp.int32(0)
        prev = jnp.int32(0)
        for s in range(n_src):
            k = lax.div(cnt[e, s] + (BLK - 1), BLK)
            for b in range(per_src):
                prev = jnp.where(b < k, s * per_src + b, prev)
                blk[e, n + b] = prev
            n = n + k
        for j in range(n_src * per_src):
            @pl.when(j >= n)
            def _():
                blk[e, j] = prev
        total[e] = n
        return carry

    lax.fori_loop(0, local_exp, listed, 0)
    load_bias.wait()
    bias[...] = braw[...].astype(F32)

    def expert(e, carry):
        slot = lax.rem(e, n_slot)
        load_w(e).wait()

        def run(rows):
            n = rows // BLK
            for j in range(n):
                b = blk[e, j]
                first = pl.multiple_of(lax.rem(b, per_src) * BLK, BLK)
                xc[j * BLK:(j + 1) * BLK, :] = xs_ref[e, lax.div(b, per_src), pl.ds(first, BLK), :]
            for n0 in range(0, width, NSTEP):
                w = min(NSTEP, width - n0)
                u = jnp.dot(xc[0:rows, :], wb[slot, :, n0:n0 + w], preferred_element_type=F32) + bias[pl.ds(e, 1), n0:n0 + w]
                uc[0:rows, n0:n0 + w] = jnp.minimum(jnp.maximum(u, LOWEST), LIMIT).astype(BF16)
            for m in range(0, width, 256):
                v = jnp.dot(uc[0:rows, m:m + 256], perm[...], preferred_element_type=F32)
                gate = v[:, :128]
                linear = jnp.maximum(v[:, 128:], -LIMIT)
                z = gate * lax.logistic(ALPHA * gate) * (linear + 1.0)
                zc[0:rows, m // 2:m // 2 + 128] = z.astype(BF16)
            for j in range(n):
                z_ref[e, pl.ds(pl.multiple_of(blk[e, j] * BLK, BLK), BLK), :] = zc[j * BLK:(j + 1) * BLK, :]

        n = total[e]

        @pl.when(jnp.logical_and(n > 0, n <= 8))
        def _():
            run(128)

        @pl.when(jnp.logical_and(n > 8, n <= 16))
        def _():
            run(256)

        @pl.when(n > 16)
        def _():
            run(384)

        @pl.when(e + n_slot < local_exp)
        def _():
            load_w(e + n_slot).start()
        return carry

    lax.fori_loop(0, local_exp, expert, 0)


def combine_kernel(z_ref, pm_hbm, wd_hbm, bd_hbm, x_hbm, out_ref,
                   bd_ref, x_ref, pm, wb, bias, yb, part, in0, in1, in2,
                   psem, lsem, wsem, s0, s1, s2, r0, r1, r2):
    local_exp, rows_all, d_ff = z_ref.shape
    n_src = 8
    cap = rows_all // n_src
    tok, d_model = x_hbm.shape
    n_col = d_model // COLS
    half = COLS // 2
    me = lax.axis_index('ep')
    barrier = pltpu.get_barrier_semaphore()
    for r in (1, 2, 4):
        pl.semaphore_signal(barrier, inc=1, device_id={'ep': flip(me, r)}, device_id_type=MESH)

    def load_w(c):
        slot = lax.rem(c, 2)
        cols = pl.ds(pl.multiple_of(c * COLS, COLS), COLS)
        return pltpu.make_async_copy(wd_hbm.at[:, :, cols], wb.at[slot], wsem.at[slot])

    load_w(0).start()
    pload = pltpu.make_async_copy(pm_hbm, pm, psem)
    pload.start()
    bload = pltpu.make_async_copy(bd_hbm, bd_ref, lsem.at[0])
    xload = pltpu.make_async_copy(x_hbm, x_ref, lsem.at[1])
    bload.start()
    xload.start()
    bload.wait()
    bias[...] = bd_ref[...].astype(F32)

    def to_mate(c):
        return remote(part.at[c, 1], in0.at[c], s0.at[c], r0.at[c], flip(me, 1))

    def to_first(c, h):
        return remote(part.at[c, 0, h, pl.ds(2, 2)], in1.at[c, h], s1.at[c, h], r1.at[c, h], flip(me, 2 + 2 * h))

    def to_second(c, h):
        return remote(part.at[c, 0, h, 1], in2.at[c, h], s2.at[c, h], r2.at[c, h], flip(me, 4 - 2 * h))

    def merge_mate(c):
        to_mate(c).wait_recv()
        for js in ((2, 3), (0, 1)):
            for h in range(2):
                for j in js:
                    part[c, 0, h, j] = part[c, 0, h, j] + in0[c, h, j]
                if js[0] == 2:
                    to_first(c, h).start()

    def merge_first(c):
        for h in range(2):
            to_first(c, h).wait_recv()
            for j in (1, 0):
                part[c, 0, h, j] = part[c, 0, h, j] + in1[c, h, j]
            to_second(c, h).start()

    def finish(c):
        for h in range(2):
            to_second(c, h).wait_recv()
            cols = pl.ds(pl.multiple_of(c * COLS + h * half, half), half)
            out_ref[:, cols] = (x_ref[:, cols].astype(F32) + (part[c, 0, h, 0] + in2[c, h])).astype(BF16)

    def step(c, carry):
        slot = lax.rem(c, 2)
        cols = pl.ds(pl.multiple_of(c * COLS, COLS), COLS)

        @pl.when(c + 1 < n_col)
        def _():
            load_w(c + 1).start()

        load_w(c).wait()
        for e in range(local_exp):
            y = jnp.dot(z_ref[e], wb[slot, e], preferred_element_type=F32) + bias[e:e + 1, cols]
            y = y.astype(BF16)
            for s in range(n_src):
                yb[s, e * cap:(e + 1) * cap, :] = y[s * cap:(s + 1) * cap, :]

        @pl.when(c == 0)
        def _():
            pload.wait()
            xload.wait()
            pl.semaphore_wait(barrier, 3)

        @pl.when(c >= 1)
        def _():
            merge_mate(c - 1)

        for core in (1, 0):
            for q in range(4):
                src = flip(me, 2 * q + core)
                sums = jnp.dot(pm[src], yb[src], preferred_element_type=F32)
                sums = (sums[2 * tok:] + sums[tok:2 * tok]) + sums[:tok]
                for h in range(2):
                    j = q if h == 1 or q in (0, 3) else 3 - q
                    part[c, core, h, j] = sums[:, h * half:(h + 1) * half]

        to_mate(c).start()

        @pl.when(c >= 2)
        def _():
            merge_first(c - 2)

        @pl.when(c >= 4)
        def _():
            finish(c - 4)
        return carry

    lax.fori_loop(0, n_col, step, 0)
    merge_mate(n_col - 1)
    for c in range(n_col - 2, n_col):
        merge_first(c)
    for c in range(n_col - 4, n_col):
        finish(c)
    for c in range(n_col):
        to_mate(c).wait_send()
        for h in range(2):
            to_first(c, h).wait_send()
            to_second(c, h).wait_send()


def solution(mesh):
    n_group = mesh.shape['ep']
    assert n_group == 8
    rows_spec = P(('dp', 'ep'), None)

    def local_block(x_in, expert_ids, norm_weight, router_w, router_b, w_gate_up, b_gate_up, w_down, b_down):
        tok, d_model = x_in.shape
        top_k = expert_ids.shape[1]
        local_exp, _, width = w_gate_up.shape
        d_ff = w_down.shape[1]
        experts = local_exp * n_group
        cap = CAPACITY_FACTOR * top_k * tok // experts
        rows_all = n_group * cap
        hbm = pl.BlockSpec(memory_space=pl.ANY)
        vmem = pl.BlockSpec(memory_space=pltpu.VMEM)
        smem = pl.BlockSpec(memory_space=pltpu.SMEM)
        dma = pltpu.SemaphoreType.DMA
        in_hbm = functools.partial(pltpu.with_memory_space_constraint, memory_space=pltpu.HBM)
        pinned = functools.partial(pltpu.with_memory_space_constraint, memory_space=pltpu.VMEM)
        xs, pm, counts = pl.pallas_call(
            functools.partial(dispatch_kernel, top_k, local_exp, cap),
            out_shape=(pltpu.VMEM((local_exp, n_group, cap, d_model), BF16),
                       pltpu.HBM((n_group, 3 * tok, local_exp * cap), BF16),
                       pltpu.HBM((local_exp, 128), jnp.int32)),
            in_specs=[hbm] * 5,
            out_specs=(vmem, hbm, hbm),
            scratch_shapes=[
                pltpu.VMEM((d_model,), BF16), pltpu.VMEM((experts, d_model), BF16), pltpu.VMEM((1, experts), BF16), pltpu.VMEM((local_exp, 128), jnp.int32),
                pltpu.VMEM((8, tok, d_model), BF16), pltpu.VMEM((8, top_k, tok), jnp.int32), pltpu.VMEM((tok, d_model), BF16),
                pltpu.VMEM((8, 128), F32), pltpu.VMEM((1, d_model), F32), pltpu.VMEM((tok, tok), BF16),
                pltpu.VMEM((8, local_exp * cap, tok), BF16), pltpu.VMEM((local_exp * cap, tok), F32),
                pltpu.VMEM((experts, tok), F32), pltpu.VMEM((8, local_exp, tok), F32),
                pltpu.VMEM((2, 3 * tok, local_exp * cap), BF16),
                dma((5,)), dma((2,)), dma((14,)), dma((8, 2)), dma((8,)), dma((8,)), dma((8,)), dma((8,))],
            compiler_params=pltpu.CompilerParams(collective_id=0, has_side_effects=True, vmem_limit_bytes=11 * MIB),
            name='dispatch',
        )(*map(in_hbm, (x_in, expert_ids.T, norm_weight, router_w.T, router_b.reshape(1, experts))))
        z = pl.pallas_call(
            gate_up_kernel,
            out_shape=pltpu.VMEM((local_exp, rows_all, d_ff), BF16),
            in_specs=[hbm, vmem, hbm, hbm],
            out_specs=vmem,
            scratch_shapes=[
                pltpu.VMEM((N_RING, d_model, width), BF16),
                pltpu.VMEM((rows_all, d_model), BF16), pltpu.VMEM((rows_all, d_ff), BF16), pltpu.VMEM((rows_all, width), BF16),
                pltpu.VMEM((local_exp, width), BF16), pltpu.VMEM((local_exp, width), F32), pltpu.VMEM((256, 256), BF16),
                pltpu.SMEM((local_exp, 128), jnp.int32), pltpu.SMEM((local_exp, 2 * rows_all // BLK), jnp.int32), pltpu.SMEM((local_exp,), jnp.int32),
                dma((N_RING,)), dma((2,))],
            compiler_params=pltpu.CompilerParams(vmem_limit_bytes=42 * MIB),
            name='gate_up',
        )(counts, pinned(xs), w_gate_up, in_hbm(b_gate_up))
        n_col = d_model // COLS
        return pl.pallas_call(
            combine_kernel,
            out_shape=pltpu.VMEM((tok, d_model), BF16),
            in_specs=[vmem, hbm, hbm, hbm, hbm],
            out_specs=vmem,
            scratch_shapes=[
                pltpu.VMEM((local_exp, d_model), BF16), pltpu.VMEM((tok, d_model), BF16),
                pltpu.VMEM((n_group, 3 * tok, local_exp * cap), BF16),
                pltpu.VMEM((2, local_exp, d_ff, COLS), BF16), pltpu.VMEM((local_exp, d_model), F32),
                pltpu.VMEM((n_group, local_exp * cap, COLS), BF16), pltpu.VMEM((n_col, 2, 2, 4, tok, COLS // 2), F32),
                pltpu.VMEM((n_col, 2, 4, tok, COLS // 2), F32), pltpu.VMEM((n_col, 2, 2, tok, COLS // 2), F32),
                pltpu.VMEM((n_col, 2, tok, COLS // 2), F32),
                dma, dma((2,)), dma((2,)), dma((n_col,)), dma((n_col, 2)), dma((n_col, 2)), dma((n_col,)), dma((n_col, 2)), dma((n_col, 2))],
            compiler_params=pltpu.CompilerParams(collective_id=1, has_side_effects=True, vmem_limit_bytes=40 * MIB),
            name='combine',
        )(pinned(z), in_hbm(pm), w_down, in_hbm(b_down), in_hbm(x_in))

    return jax.shard_map(local_block, mesh=mesh, in_specs=(rows_spec, rows_spec, P(), P(), P(), P('ep', None, None), P('ep', None), P('ep', None, None), P('ep', None)), out_specs=rows_spec, check_vma=False)
```

```python
import functools

import jax
import jax.numpy as jnp
from jax import lax
from jax.experimental import pallas as pl
from jax.experimental.pallas import tpu as pltpu
from jax.sharding import PartitionSpec as P

CAPACITY_FACTOR = 4
EPSILON = 1e-5
LIMIT = 7.0
ALPHA = 1.702
LOWEST = -3.3895313892515355e38
BLK = 16
COLS = 256
MESH = pl.DeviceIdType.MESH
F32 = jnp.float32
BF16 = jnp.bfloat16
MIB = 1024 * 1024
N_RING = 3
NSTEP = 1536


def flip(me, role):
    core = lax.rem(lax.rem(me, 2) + lax.rem(role, 2), 2)
    x = lax.rem(lax.rem(lax.div(me, 2), 2) + lax.rem(lax.div(role, 2), 2), 2)
    y = lax.rem(lax.div(me, 4) + lax.div(role, 4), 2)
    return y * 4 + x * 2 + core


def remote(src, dst, send, recv, device):
    return pltpu.make_async_remote_copy(src_ref=src, dst_ref=dst, send_sem=send, recv_sem=recv, device_id={'ep': device}, device_id_type=MESH)


def dispatch_kernel(top_k, local_exp, cap, x_hbm, ids_hbm, g_hbm, wr_hbm, br_hbm, wgu_hbm, xs_ref, wpre_ref, pm_hbm, cnt_hbm,
                    g_ref, wr_ref, br_ref, cnt_ref, xb, idb, hb, brp, gain, tri, oh, pt, probs, prb, pstage,
                    lsem, psem, ssem, rsem, isend, irecv, gsend, grecv, wsem):
    tok, d_model = x_hbm.shape
    experts = wr_ref.shape[0]
    half = tok // 2
    me = lax.axis_index('ep')
    load_x = pltpu.make_async_copy(x_hbm, xb.at[0], lsem.at[0])
    load_ids = pltpu.make_async_copy(ids_hbm, idb.at[0], lsem.at[1])
    load_x.start()
    load_ids.start()
    small = [pltpu.make_async_copy(a, b, lsem.at[k + 2]) for k, (a, b) in enumerate([(g_hbm, g_ref), (wr_hbm, wr_ref), (br_hbm, br_ref)])]
    for c in small:
        c.start()
    barrier = pltpu.get_barrier_semaphore()
    for r in range(1, 8):
        pl.semaphore_signal(barrier, inc=1, device_id={'ep': flip(me, r)}, device_id_type=MESH)
    load_x.wait()
    load_ids.wait()
    pl.semaphore_wait(barrier, 7)

    def piece(src_role, h, dst_role, to_role, k):
        rows = pl.ds(h * half, half)
        return remote(xb.at[src_role, rows], xb.at[dst_role, rows], ssem.at[k], rsem.at[dst_role, h], flip(me, to_role))

    def landed(role, h):
        piece(role, h, role, 1, 0).wait_recv()

    sends = [(0, 0, 2, 2), (0, 1, 4, 4), (0, 0, 1, 1), (0, 1, 1, 1), (0, 1, 2, 2), (0, 0, 4, 4)]
    relays = [(2, 0, 6, 4), (2, 0, 3, 1), (4, 1, 6, 2), (4, 1, 5, 1), (2, 1, 3, 1), (4, 0, 5, 1)]
    last = [(6, 0, 7, 1), (6, 1, 7, 1)]
    everything = sends + relays + last

    def go(k):
        piece(*everything[k], k).start()

    for k in range(6):
        go(k)
    fetch = [pltpu.make_async_copy(wgu_hbm.at[e], wpre_ref.at[e], wsem.at[e]) for e in range(wpre_ref.shape[0])]
    for c in fetch:
        c.start()
    ids_out = [remote(idb.at[0], idb.at[r], isend.at[r], irecv.at[r], flip(me, r)) for r in range(1, 8)]
    for c in ids_out:
        c.start()

    for c in small:
        c.wait()
    brp[...] = jnp.zeros_like(brp)
    brp[0:1, :experts] = br_ref[...].astype(F32)
    bias = jnp.transpose(jnp.broadcast_to(brp[0:1, :], (tok, tok)))[:experts]
    gain[...] = g_ref[...].astype(F32).reshape(gain.shape)
    tri[...] = (lax.broadcasted_iota(jnp.int32, (tok, tok), 0) < lax.broadcasted_iota(jnp.int32, (tok, tok), 1)).astype(F32).astype(BF16)
    cnt_ref[...] = jnp.zeros_like(cnt_ref)

    def normed(i):
        def norm(j, c):
            rows = pl.ds(pl.multiple_of(j * 64, 64), 64)
            xf = xb[i, rows, :].astype(F32)
            inv = lax.rsqrt(jnp.mean(xf * xf, axis=-1, keepdims=True) + EPSILON)
            hb[rows, :] = (xf * inv * gain[...]).astype(BF16)
            return c

        lax.fori_loop(0, tok // 64, norm, 0)

    normed(0)
    logits = lax.dot_general(wr_ref[...], hb[...], (((1,), (1,)), ((), ())), preferred_element_type=F32) + bias
    expert_no = lax.broadcasted_iota(jnp.int32, (experts, tok), 0)
    chosen = jnp.zeros((experts, tok), F32)
    for k in range(top_k):
        chosen = jnp.where(expert_no == idb[0, k:k + 1, :], 1.0, chosen)
    picked = jnp.where(chosen > 0, logits, -jnp.inf)
    ex = jnp.exp(picked - jnp.max(picked, axis=0, keepdims=True))
    probs[...] = ex / jnp.sum(ex, axis=0, keepdims=True)

    def block(device):
        return probs.at[pl.ds(pl.multiple_of(device * local_exp, local_exp), local_exp)]

    gates_out = [remote(block(flip(me, r)), prb.at[r], gsend.at[r], grecv.at[r], flip(me, r)) for r in range(1, 8)]
    for c in gates_out:
        c.start()
    prb[0] = probs[pl.ds(pl.multiple_of(me * local_exp, local_exp), local_exp), :]

    def plan(i, carry):
        @pl.when(i >= 1)
        def _():
            remote(idb.at[i], idb.at[i], isend.at[0], irecv.at[i], flip(me, 1)).wait_recv()
            remote(prb.at[i], prb.at[i], gsend.at[0], grecv.at[i], flip(me, 1)).wait_recv()

        @pl.when(i == 3)
        def _():
            landed(2, 0)
            go(6)
            go(7)
            landed(4, 1)
            go(8)
            go(9)

        src = flip(me, i)
        slot = lax.rem(i, 2)
        out_p = pltpu.make_async_copy(pstage.at[slot], pm_hbm.at[src], psem.at[slot])
        ids = idb[i]
        number = me * local_exp + lax.broadcasted_iota(jnp.int32, (local_exp, tok), 0)
        held = jnp.zeros((local_exp, tok), F32)
        for k in range(top_k):
            held = jnp.where(number == ids[k:k + 1, :], 1.0, held)
        rank = jnp.dot(held.astype(BF16), tri[...], preferred_element_type=F32)
        count = jnp.sum(held, axis=1, keepdims=True)
        lane = lax.broadcasted_iota(jnp.int32, cnt_ref.shape, 1)
        cnt_ref[...] = jnp.where(lane == src, count.astype(jnp.int32), cnt_ref[...])
        rank = jnp.where(held > 0, rank, -1.0)
        place = lax.broadcasted_iota(jnp.int32, (cap, tok), 0).astype(F32)
        p_loc = prb[i]
        for e in range(local_exp):
            hit = rank[e:e + 1, :] == place
            oh[i, e * cap:(e + 1) * cap, :] = jnp.where(hit, 1.0, 0.0).astype(BF16)
            pt[e * cap:(e + 1) * cap, :] = jnp.where(hit, p_loc[e:e + 1, :], 0.0)

        @pl.when(i >= 2)
        def _():
            out_p.wait()

        for b in range(local_exp * cap // tok):
            p = jnp.transpose(pt[b * tok:(b + 1) * tok, :])
            for part in range(3):
                low = p.astype(BF16)
                pstage[slot, part * tok:(part + 1) * tok, b * tok:(b + 1) * tok] = low
                p = p - low.astype(F32)
        out_p.start()
        return carry

    lax.fori_loop(0, 8, plan, 0)
    save_cnt = pltpu.make_async_copy(cnt_ref, cnt_hbm, lsem.at[0])
    save_cnt.start()

    def gather(i, carry):
        @pl.when(i == 1)
        def _():
            landed(1, 0)
            landed(1, 1)

        @pl.when(i == 2)
        def _():
            landed(2, 1)
            go(10)
            landed(4, 0)
            go(11)

        @pl.when(i == 3)
        def _():
            landed(3, 0)
            landed(3, 1)

        @pl.when(i == 5)
        def _():
            landed(5, 0)
            landed(5, 1)

        @pl.when(i == 6)
        def _():
            landed(6, 0)
            go(12)
            landed(6, 1)
            go(13)

        @pl.when(i == 7)
        def _():
            landed(7, 0)
            landed(7, 1)

        normed(i)
        src = flip(me, i)
        for n in range(0, d_model, 512):
            rows = jnp.dot(oh[i], hb[:, n:n + 512], preferred_element_type=F32).astype(BF16)
            for e in range(local_exp):
                xs_ref[e, src, :, n:n + 512] = rows[e * cap:(e + 1) * cap, :]
        return carry

    lax.fori_loop(0, 8, gather, 0)
    save_cnt.wait()
    for slot in range(2):
        pltpu.make_async_copy(pstage.at[slot], pm_hbm.at[me], psem.at[slot]).wait()
    for c in fetch:
        c.wait()
    for c in ids_out + gates_out:
        c.wait_send()
    for k in range(len(everything)):
        piece(*everything[k], k).wait_send()


def gate_up_kernel(cnt_hbm, xs_ref, wpre_ref, wgu_hbm, bgu_hbm, z_ref, wb, xc, uc, braw, bias, perm, cnt, blk, total, wsem, sem):
    local_exp, n_src, cap, d_model = xs_ref.shape
    width = wgu_hbm.shape[2]
    per_src = cap // BLK
    n_slot = wb.shape[0]

    steps = [(n0, min(NSTEP, width - n0)) for n0 in range(0, width, NSTEP)]

    def load_w(e, p):
        slot = lax.rem(e, n_slot)
        cols = pl.ds(*steps[p])
        return pltpu.make_async_copy(wgu_hbm.at[e, :, cols], wb.at[slot, :, cols], wsem.at[slot, p])

    load_cnt = pltpu.make_async_copy(cnt_hbm, cnt, sem.at[0])
    load_bias = pltpu.make_async_copy(bgu_hbm, braw, sem.at[1])
    load_cnt.start()
    load_bias.start()
    row = lax.broadcasted_iota(jnp.int32, perm.shape, 0)
    col = lax.broadcasted_iota(jnp.int32, perm.shape, 1)
    source = jnp.where(col < 128, 2 * col, 2 * col - 255)
    perm[...] = jnp.where(row == source, 1.0, 0.0).astype(BF16)
    load_cnt.wait()

    def listed(e, carry):
        z_ref[e] = jnp.zeros(z_ref.shape[1:], BF16)
        n = jnp.int32(0)
        prev = jnp.int32(0)
        for s in range(n_src):
            k = lax.div(cnt[e, s] + (BLK - 1), BLK)
            for b in range(per_src):
                prev = jnp.where(b < k, s * per_src + b, prev)
                blk[e, n + b] = prev
            n = n + k
        for j in range(n_src * per_src):
            @pl.when(j >= n)
            def _():
                blk[e, j] = prev
        total[e] = n
        return carry

    lax.fori_loop(0, local_exp, listed, 0)
    load_bias.wait()
    bias[...] = braw[...].astype(F32)

    def expert(e, carry):
        slot = lax.rem(e, n_slot)
        def run(rows):
            n = rows // BLK
            for j in range(n):
                b = blk[e, j]
                first = pl.multiple_of(lax.rem(b, per_src) * BLK, BLK)
                xc[j * BLK:(j + 1) * BLK, :] = xs_ref[e, lax.div(b, per_src), pl.ds(first, BLK), :]
            for p, (n0, w) in enumerate(steps):
                @pl.when(e >= n_slot)
                def _():
                    load_w(e, p).wait()

                u = jnp.dot(xc[0:rows, :], wb[slot, :, n0:n0 + w], preferred_element_type=F32) + bias[pl.ds(e, 1), n0:n0 + w]
                uc[0:rows, n0:n0 + w] = jnp.minimum(jnp.maximum(u, LOWEST), LIMIT).astype(BF16)

                @pl.when(e + n_slot < local_exp)
                def _():
                    load_w(e + n_slot, p).start()

            for m in range(0, width, 256):
                v = jnp.dot(uc[0:rows, m:m + 256], perm[...], preferred_element_type=F32)
                gate = v[:, :128]
                linear = jnp.maximum(v[:, 128:], -LIMIT)
                z = gate * lax.logistic(ALPHA * gate) * (linear + 1.0)
                z = z.astype(BF16)
                for j in range(n):
                    z_ref[e, pl.ds(pl.multiple_of(blk[e, j] * BLK, BLK), BLK), m // 2:m // 2 + 128] = z[j * BLK:(j + 1) * BLK, :]

        n = total[e]

        @pl.when(jnp.logical_and(n > 0, n <= 8))
        def _():
            run(128)

        @pl.when(jnp.logical_and(n > 8, n <= 16))
        def _():
            run(256)

        @pl.when(n > 16)
        def _():
            run(384)

        @pl.when(n == 0)
        def _():
            for p in range(len(steps)):
                @pl.when(e >= n_slot)
                def _():
                    load_w(e, p).wait()

                @pl.when(e + n_slot < local_exp)
                def _():
                    load_w(e + n_slot, p).start()
        return carry

    lax.fori_loop(0, local_exp, expert, 0)


def combine_kernel(z_ref, pm_hbm, wd_hbm, bd_hbm, x_hbm, out_ref,
                   bd_ref, x_ref, pm, wb, bias, yb, part, in0, in1, in2,
                   psem, lsem, wsem, s0, s1, s2, r0, r1, r2):
    local_exp, rows_all, d_ff = z_ref.shape
    n_src = 8
    cap = rows_all // n_src
    tok, d_model = x_hbm.shape
    n_col = d_model // COLS
    half = COLS // 2
    me = lax.axis_index('ep')
    barrier = pltpu.get_barrier_semaphore()
    for r in (1, 2, 4):
        pl.semaphore_signal(barrier, inc=1, device_id={'ep': flip(me, r)}, device_id_type=MESH)

    few = local_exp // 2

    def load_w(c, g):
        slot = lax.rem(c, 2)
        cols = pl.ds(pl.multiple_of(c * COLS, COLS), COLS)
        group = pl.ds(g * few, few)
        return pltpu.make_async_copy(wd_hbm.at[group, :, cols], wb.at[slot, group], wsem.at[slot, g])

    load_w(0, 0).start()
    load_w(0, 1).start()
    pload = pltpu.make_async_copy(pm_hbm, pm, psem)
    pload.start()
    bload = pltpu.make_async_copy(bd_hbm, bd_ref, lsem.at[0])
    xload = pltpu.make_async_copy(x_hbm, x_ref, lsem.at[1])
    bload.start()
    xload.start()
    bload.wait()
    bias[...] = bd_ref[...].astype(F32)

    def to_mate(c):
        return remote(part.at[c, 1], in0.at[c], s0.at[c], r0.at[c], flip(me, 1))

    def to_first(c, h):
        return remote(part.at[c, 0, h, pl.ds(2, 2)], in1.at[c, h], s1.at[c, h], r1.at[c, h], flip(me, 2 + 2 * h))

    def to_second(c, h):
        return remote(part.at[c, 0, h, 1], in2.at[c, h], s2.at[c, h], r2.at[c, h], flip(me, 4 - 2 * h))

    def merge_mate(c):
        to_mate(c).wait_recv()
        for js in ((2, 3), (0, 1)):
            for h in range(2):
                for j in js:
                    part[c, 0, h, j] = part[c, 0, h, j] + in0[c, h, j]
                if js[0] == 2:
                    to_first(c, h).start()

    def merge_first(c):
        for h in range(2):
            to_first(c, h).wait_recv()
            for j in (1, 0):
                part[c, 0, h, j] = part[c, 0, h, j] + in1[c, h, j]
            to_second(c, h).start()

    def finish(c):
        for h in range(2):
            to_second(c, h).wait_recv()
            cols = pl.ds(pl.multiple_of(c * COLS + h * half, half), half)
            out_ref[:, cols] = (x_ref[:, cols].astype(F32) + (part[c, 0, h, 0] + in2[c, h])).astype(BF16)

    def step(c, carry):
        slot = lax.rem(c, 2)
        cols = pl.ds(pl.multiple_of(c * COLS, COLS), COLS)

        @pl.when(c + 1 < n_col)
        def _():
            load_w(c + 1, 0).start()
            load_w(c + 1, 1).start()

        for g in range(2):
            load_w(c, g).wait()
            if g == 1:
                @pl.when(c == 0)
                def _():
                    pload.wait()
                    xload.wait()
                    pl.semaphore_wait(barrier, 3)

                @pl.when(c >= 1)
                def _():
                    merge_mate(c - 1)

            for e in range(g * few, (g + 1) * few):
                y = jnp.dot(z_ref[e], wb[slot, e], preferred_element_type=F32) + bias[e:e + 1, cols]
                y = y.astype(BF16)
                for s in range(n_src):
                    yb[s, e * cap:(e + 1) * cap, :] = y[s * cap:(s + 1) * cap, :]

        for core in (1, 0):
            for q in range(4):
                src = flip(me, 2 * q + core)
                sums = jnp.dot(pm[src], yb[src], preferred_element_type=F32)
                sums = (sums[2 * tok:] + sums[tok:2 * tok]) + sums[:tok]
                for h in range(2):
                    j = q if h == 1 or q in (0, 3) else 3 - q
                    part[c, core, h, j] = sums[:, h * half:(h + 1) * half]
            if core == 1:
                to_mate(c).start()

        @pl.when(c >= 2)
        def _():
            merge_first(c - 2)

        @pl.when(c >= 4)
        def _():
            finish(c - 4)
        return carry

    lax.fori_loop(0, n_col, step, 0)
    merge_mate(n_col - 1)
    for c in range(n_col - 2, n_col):
        merge_first(c)
    for c in range(n_col - 4, n_col):
        finish(c)
    for c in range(n_col):
        to_mate(c).wait_send()
        for h in range(2):
            to_first(c, h).wait_send()
            to_second(c, h).wait_send()


def solution(mesh):
    n_group = mesh.shape['ep']
    assert n_group == 8
    rows_spec = P(('dp', 'ep'), None)

    def local_block(x_in, expert_ids, norm_weight, router_w, router_b, w_gate_up, b_gate_up, w_down, b_down):
        tok, d_model = x_in.shape
        top_k = expert_ids.shape[1]
        local_exp, _, width = w_gate_up.shape
        d_ff = w_down.shape[1]
        experts = local_exp * n_group
        cap = CAPACITY_FACTOR * top_k * tok // experts
        rows_all = n_group * cap
        hbm = pl.BlockSpec(memory_space=pl.ANY)
        vmem = pl.BlockSpec(memory_space=pltpu.VMEM)
        smem = pl.BlockSpec(memory_space=pltpu.SMEM)
        dma = pltpu.SemaphoreType.DMA
        in_hbm = functools.partial(pltpu.with_memory_space_constraint, memory_space=pltpu.HBM)
        pinned = functools.partial(pltpu.with_memory_space_constraint, memory_space=pltpu.VMEM)
        xs, w_first, pm, counts = pl.pallas_call(
            functools.partial(dispatch_kernel, top_k, local_exp, cap),
            out_shape=(pltpu.VMEM((local_exp, n_group, cap, d_model), BF16),
                       pltpu.VMEM((N_RING, d_model, width), BF16),
                       pltpu.HBM((n_group, 3 * tok, local_exp * cap), BF16),
                       pltpu.HBM((local_exp, 128), jnp.int32)),
            in_specs=[hbm] * 6,
            out_specs=(vmem, vmem, hbm, hbm),
            scratch_shapes=[
                pltpu.VMEM((d_model,), BF16), pltpu.VMEM((experts, d_model), BF16), pltpu.VMEM((1, experts), BF16), pltpu.VMEM((local_exp, 128), jnp.int32),
                pltpu.VMEM((8, tok, d_model), BF16), pltpu.VMEM((8, top_k, tok), jnp.int32), pltpu.VMEM((tok, d_model), BF16),
                pltpu.VMEM((8, 128), F32), pltpu.VMEM((1, d_model), F32), pltpu.VMEM((tok, tok), BF16),
                pltpu.VMEM((8, local_exp * cap, tok), BF16), pltpu.VMEM((local_exp * cap, tok), F32),
                pltpu.VMEM((experts, tok), F32), pltpu.VMEM((8, local_exp, tok), F32),
                pltpu.VMEM((2, 3 * tok, local_exp * cap), BF16),
                dma((5,)), dma((2,)), dma((14,)), dma((8, 2)), dma((8,)), dma((8,)), dma((8,)), dma((8,)), dma((N_RING,))],
            compiler_params=pltpu.CompilerParams(collective_id=0, has_side_effects=True, vmem_limit_bytes=10 * MIB),
            name='dispatch',
        )(*map(in_hbm, (x_in, expert_ids.T, norm_weight, router_w.T, router_b.reshape(1, experts), w_gate_up)))
        z, _ = pl.pallas_call(
            gate_up_kernel,
            out_shape=(pltpu.VMEM((local_exp, rows_all, d_ff), BF16), pltpu.VMEM((N_RING, d_model, width), BF16)),
            in_specs=[hbm, vmem, vmem, hbm, hbm],
            out_specs=(vmem, vmem),
            input_output_aliases={2: 1},
            scratch_shapes=[
                pltpu.VMEM((rows_all, d_model), BF16), pltpu.VMEM((rows_all, width), BF16),
                pltpu.VMEM((local_exp, width), BF16), pltpu.VMEM((local_exp, width), F32), pltpu.VMEM((256, 256), BF16),
                pltpu.SMEM((local_exp, 128), jnp.int32), pltpu.SMEM((local_exp, 2 * rows_all // BLK), jnp.int32), pltpu.SMEM((local_exp,), jnp.int32),
                dma((N_RING, -(-width // NSTEP))), dma((2,))],
            compiler_params=pltpu.CompilerParams(vmem_limit_bytes=10 * MIB),
            name='gate_up',
        )(counts, pinned(xs), pinned(w_first), w_gate_up, in_hbm(b_gate_up))
        n_col = d_model // COLS
        return pl.pallas_call(
            combine_kernel,
            out_shape=pltpu.VMEM((tok, d_model), BF16),
            in_specs=[vmem, hbm, hbm, hbm, hbm],
            out_specs=vmem,
            scratch_shapes=[
                pltpu.VMEM((local_exp, d_model), BF16), pltpu.VMEM((tok, d_model), BF16),
                pltpu.VMEM((n_group, 3 * tok, local_exp * cap), BF16),
                pltpu.VMEM((2, local_exp, d_ff, COLS), BF16), pltpu.VMEM((local_exp, d_model), F32),
                pltpu.VMEM((n_group, local_exp * cap, COLS), BF16), pltpu.VMEM((n_col, 2, 2, 4, tok, COLS // 2), F32),
                pltpu.VMEM((n_col, 2, 4, tok, COLS // 2), F32), pltpu.VMEM((n_col, 2, 2, tok, COLS // 2), F32),
                pltpu.VMEM((n_col, 2, tok, COLS // 2), F32),
                dma, dma((2,)), dma((2, 2)), dma((n_col,)), dma((n_col, 2)), dma((n_col, 2)), dma((n_col,)), dma((n_col, 2)), dma((n_col, 2))],
            compiler_params=pltpu.CompilerParams(collective_id=1, has_side_effects=True, vmem_limit_bytes=55 * MIB),
            name='combine',
        )(pinned(z), in_hbm(pm), w_down, in_hbm(b_down), in_hbm(x_in))

    return jax.shard_map(local_block, mesh=mesh, in_specs=(rows_spec, rows_spec, P(), P(), P(), P('ep', None, None), P('ep', None), P('ep', None, None), P('ep', None)), out_specs=rows_spec, check_vma=False)
```

```python
import functools

import jax
import jax.numpy as jnp
from jax import lax
from jax.experimental import pallas as pl
from jax.experimental.pallas import tpu as pltpu
from jax.sharding import PartitionSpec as P

CAPACITY_FACTOR = 4
EPSILON = 1e-5
LIMIT = 7.0
ALPHA = 1.702
LOWEST = -3.3895313892515355e38
BLK = 16
COLS = 256
MESH = pl.DeviceIdType.MESH
F32 = jnp.float32
BF16 = jnp.bfloat16
MIB = 1024 * 1024
N_RING = 3
NSTEP = 1536


def flip(me, role):
    core = lax.rem(lax.rem(me, 2) + lax.rem(role, 2), 2)
    x = lax.rem(lax.rem(lax.div(me, 2), 2) + lax.rem(lax.div(role, 2), 2), 2)
    y = lax.rem(lax.div(me, 4) + lax.div(role, 4), 2)
    return y * 4 + x * 2 + core


def remote(src, dst, send, recv, device):
    return pltpu.make_async_remote_copy(src_ref=src, dst_ref=dst, send_sem=send, recv_sem=recv, device_id={'ep': device}, device_id_type=MESH)


def dispatch_kernel(top_k, local_exp, cap, x_hbm, ids_hbm, g_hbm, wr_hbm, br_hbm, wgu_hbm, xs_ref, wpre_ref, pm_hbm, cnt_hbm,
                    g_ref, wr_ref, br_ref, cnt_ref, xb, idb, hb, brp, gain, tri, oh, pt, probs, prb, pstage,
                    lsem, psem, ssem, rsem, isend, irecv, gsend, grecv, wsem):
    tok, d_model = x_hbm.shape
    experts = wr_ref.shape[0]
    half = tok // 2
    me = lax.axis_index('ep')
    load_x = pltpu.make_async_copy(x_hbm, xb.at[0], lsem.at[0])
    load_ids = pltpu.make_async_copy(ids_hbm, idb.at[0], lsem.at[1])
    load_x.start()
    load_ids.start()
    small = [pltpu.make_async_copy(a, b, lsem.at[k + 2]) for k, (a, b) in enumerate([(g_hbm, g_ref), (wr_hbm, wr_ref), (br_hbm, br_ref)])]
    for c in small:
        c.start()
    barrier = pltpu.get_barrier_semaphore()
    for r in range(1, 8):
        pl.semaphore_signal(barrier, inc=1, device_id={'ep': flip(me, r)}, device_id_type=MESH)
    load_x.wait()
    load_ids.wait()
    pl.semaphore_wait(barrier, 7)

    def piece(src_role, h, dst_role, to_role, k):
        rows = pl.ds(h * half, half)
        return remote(xb.at[src_role, rows], xb.at[dst_role, rows], ssem.at[k], rsem.at[dst_role, h], flip(me, to_role))

    def landed(role, h):
        piece(role, h, role, 1, 0).wait_recv()

    sends = [(0, 0, 2, 2), (0, 1, 4, 4), (0, 0, 1, 1), (0, 1, 1, 1), (0, 1, 2, 2), (0, 0, 4, 4)]
    relays = [(2, 0, 6, 4), (2, 0, 3, 1), (4, 1, 6, 2), (4, 1, 5, 1), (2, 1, 3, 1), (4, 0, 5, 1)]
    last = [(6, 0, 7, 1), (6, 1, 7, 1)]
    everything = sends + relays + last

    def go(k):
        piece(*everything[k], k).start()

    ids_out = [remote(idb.at[0], idb.at[r], isend.at[r], irecv.at[r], flip(me, r)) for r in range(1, 8)]
    for c in ids_out:
        c.start()
    for k in range(4):
        go(k)
    fetch = [pltpu.make_async_copy(wgu_hbm.at[e], wpre_ref.at[e], wsem.at[e]) for e in range(wpre_ref.shape[0])]
    for c in fetch:
        c.start()
    for c in small:
        c.wait()
    brp[...] = jnp.zeros_like(brp)
    brp[0:1, :experts] = br_ref[...].astype(F32)
    bias = jnp.transpose(jnp.broadcast_to(brp[0:1, :], (tok, tok)))[:experts]
    gain[...] = g_ref[...].astype(F32).reshape(gain.shape)
    tri[...] = (lax.broadcasted_iota(jnp.int32, (tok, tok), 0) < lax.broadcasted_iota(jnp.int32, (tok, tok), 1)).astype(F32).astype(BF16)
    cnt_ref[...] = jnp.zeros_like(cnt_ref)

    def normed(i):
        def norm(j, c):
            rows = pl.ds(pl.multiple_of(j * 64, 64), 64)
            xf = xb[i, rows, :].astype(F32)
            inv = lax.rsqrt(jnp.mean(xf * xf, axis=-1, keepdims=True) + EPSILON)
            hb[rows, :] = (xf * inv * gain[...]).astype(BF16)
            return c

        lax.fori_loop(0, tok // 64, norm, 0)

    normed(0)
    logits = lax.dot_general(wr_ref[...], hb[...], (((1,), (1,)), ((), ())), preferred_element_type=F32) + bias
    expert_no = lax.broadcasted_iota(jnp.int32, (experts, tok), 0)
    chosen = jnp.zeros((experts, tok), F32)
    for k in range(top_k):
        chosen = jnp.where(expert_no == idb[0, k:k + 1, :], 1.0, chosen)
    picked = jnp.where(chosen > 0, logits, -jnp.inf)
    ex = jnp.exp(picked - jnp.max(picked, axis=0, keepdims=True))
    probs[...] = ex / jnp.sum(ex, axis=0, keepdims=True)

    def block(device):
        return probs.at[pl.ds(pl.multiple_of(device * local_exp, local_exp), local_exp)]

    gates_out = [remote(block(flip(me, r)), prb.at[r], gsend.at[r], grecv.at[r], flip(me, r)) for r in range(1, 8)]
    for c in gates_out:
        c.start()
    go(4)
    go(5)
    prb[0] = probs[pl.ds(pl.multiple_of(me * local_exp, local_exp), local_exp), :]

    def seat(i, carry):
        @pl.when(i >= 1)
        def _():
            remote(idb.at[i], idb.at[i], isend.at[0], irecv.at[i], flip(me, 1)).wait_recv()

        src = flip(me, i)
        ids = idb[i]
        number = me * local_exp + lax.broadcasted_iota(jnp.int32, (local_exp, tok), 0)
        held = jnp.zeros((local_exp, tok), F32)
        for k in range(top_k):
            held = jnp.where(number == ids[k:k + 1, :], 1.0, held)
        rank = jnp.dot(held.astype(BF16), tri[...], preferred_element_type=F32)
        count = jnp.sum(held, axis=1, keepdims=True)
        lane = lax.broadcasted_iota(jnp.int32, cnt_ref.shape, 1)
        cnt_ref[...] = jnp.where(lane == src, count.astype(jnp.int32), cnt_ref[...])
        rank = jnp.where(held > 0, rank, -1.0)
        place = lax.broadcasted_iota(jnp.int32, (cap, tok), 0).astype(F32)
        for e in range(local_exp):
            oh[i, e * cap:(e + 1) * cap, :] = jnp.where(rank[e:e + 1, :] == place, 1.0, 0.0).astype(BF16)
        return carry

    lax.fori_loop(0, 8, seat, 0)
    landed(2, 0)
    go(6)
    go(7)
    landed(4, 1)
    go(8)
    go(9)

    def weigh(i, carry):
        @pl.when(i >= 1)
        def _():
            remote(prb.at[i], prb.at[i], gsend.at[0], grecv.at[i], flip(me, 1)).wait_recv()

        slot = lax.rem(i, 2)
        out_p = pltpu.make_async_copy(pstage.at[slot], pm_hbm.at[flip(me, i)], psem.at[slot])
        p_loc = prb[i]
        for e in range(local_exp):
            hit = oh[i, e * cap:(e + 1) * cap, :].astype(F32) > 0
            pt[e * cap:(e + 1) * cap, :] = jnp.where(hit, p_loc[e:e + 1, :], 0.0)

        @pl.when(i >= 2)
        def _():
            out_p.wait()

        for b in range(local_exp * cap // tok):
            p = jnp.transpose(pt[b * tok:(b + 1) * tok, :])
            for part in range(3):
                low = p.astype(BF16)
                pstage[slot, part * tok:(part + 1) * tok, b * tok:(b + 1) * tok] = low
                p = p - low.astype(F32)
        out_p.start()
        return carry

    lax.fori_loop(0, 8, weigh, 0)
    save_cnt = pltpu.make_async_copy(cnt_ref, cnt_hbm, lsem.at[0])
    save_cnt.start()

    def gather(i, carry):
        @pl.when(i == 1)
        def _():
            landed(1, 0)
            landed(1, 1)

        @pl.when(i == 2)
        def _():
            landed(2, 1)
            go(10)
            landed(4, 0)
            go(11)

        @pl.when(i == 3)
        def _():
            landed(3, 0)
            landed(3, 1)

        @pl.when(i == 5)
        def _():
            landed(5, 0)
            landed(5, 1)

        @pl.when(i == 6)
        def _():
            landed(6, 0)
            go(12)
            landed(6, 1)
            go(13)

        @pl.when(i == 7)
        def _():
            landed(7, 0)
            landed(7, 1)

        normed(i)
        src = flip(me, i)
        for n in range(0, d_model, 512):
            rows = jnp.dot(oh[i], hb[:, n:n + 512], preferred_element_type=F32).astype(BF16)
            for e in range(local_exp):
                xs_ref[e, src, :, n:n + 512] = rows[e * cap:(e + 1) * cap, :]
        return carry

    lax.fori_loop(0, 8, gather, 0)
    save_cnt.wait()
    for slot in range(2):
        pltpu.make_async_copy(pstage.at[slot], pm_hbm.at[me], psem.at[slot]).wait()
    for c in fetch:
        c.wait()
    for c in ids_out + gates_out:
        c.wait_send()
    for k in range(len(everything)):
        piece(*everything[k], k).wait_send()


def gate_up_kernel(cnt_hbm, xs_ref, wpre_ref, wgu_hbm, bgu_hbm, z_ref, wb, xc, uc, braw, bias, perm, cnt, blk, total, wsem, sem):
    local_exp, n_src, cap, d_model = xs_ref.shape
    width = wgu_hbm.shape[2]
    per_src = cap // BLK
    n_slot = wb.shape[0]

    steps = [(n0, min(NSTEP, width - n0)) for n0 in range(0, width, NSTEP)]

    def load_w(e, p):
        slot = lax.rem(e, n_slot)
        cols = pl.ds(*steps[p])
        return pltpu.make_async_copy(wgu_hbm.at[e, :, cols], wb.at[slot, :, cols], wsem.at[slot, p])

    load_cnt = pltpu.make_async_copy(cnt_hbm, cnt, sem.at[0])
    load_bias = pltpu.make_async_copy(bgu_hbm, braw, sem.at[1])
    load_cnt.start()
    load_bias.start()
    row = lax.broadcasted_iota(jnp.int32, perm.shape, 0)
    col = lax.broadcasted_iota(jnp.int32, perm.shape, 1)
    source = jnp.where(col < 128, 2 * col, 2 * col - 255)
    perm[...] = jnp.where(row == source, 1.0, 0.0).astype(BF16)

    def clear(e, carry):
        z_ref[e] = jnp.zeros(z_ref.shape[1:], BF16)
        return carry

    lax.fori_loop(0, local_exp, clear, 0)
    load_cnt.wait()

    def listed(e, carry):
        n = jnp.int32(0)
        prev = jnp.int32(0)
        for s in range(n_src):
            k = lax.div(cnt[e, s] + (BLK - 1), BLK)
            for b in range(per_src):
                prev = jnp.where(b < k, s * per_src + b, prev)
                blk[e, n + b] = prev
            n = n + k
        for j in range(n_src * per_src):
            blk[e, n + j] = prev
        total[e] = n
        return carry

    lax.fori_loop(0, local_exp, listed, 0)
    load_bias.wait()
    bias[...] = braw[...].astype(F32)

    def expert(e, carry):
        slot = lax.rem(e, n_slot)
        def run(rows):
            n = rows // BLK
            for j in range(n):
                b = blk[e, j]
                first = pl.multiple_of(lax.rem(b, per_src) * BLK, BLK)
                xc[j * BLK:(j + 1) * BLK, :] = xs_ref[e, lax.div(b, per_src), pl.ds(first, BLK), :]
            for p, (n0, w) in enumerate(steps):
                @pl.when(e >= n_slot)
                def _():
                    load_w(e, p).wait()

                u = jnp.dot(xc[0:rows, :], wb[slot, :, n0:n0 + w], preferred_element_type=F32) + bias[pl.ds(e, 1), n0:n0 + w]
                uc[0:rows, n0:n0 + w] = jnp.minimum(jnp.maximum(u, LOWEST), LIMIT).astype(BF16)

                @pl.when(e + n_slot < local_exp)
                def _():
                    load_w(e + n_slot, p).start()

            for m in range(0, width, 256):
                v = jnp.dot(uc[0:rows, m:m + 256], perm[...], preferred_element_type=F32)
                gate = v[:, :128]
                linear = jnp.maximum(v[:, 128:], -LIMIT)
                z = gate * lax.logistic(ALPHA * gate) * (linear + 1.0)
                z = z.astype(BF16)
                for j in range(n):
                    z_ref[e, pl.ds(pl.multiple_of(blk[e, j] * BLK, BLK), BLK), m // 2:m // 2 + 128] = z[j * BLK:(j + 1) * BLK, :]

        n = total[e]

        @pl.when(jnp.logical_and(n > 0, n <= 8))
        def _():
            run(128)

        @pl.when(jnp.logical_and(n > 8, n <= 16))
        def _():
            run(256)

        @pl.when(n > 16)
        def _():
            run(384)

        @pl.when(n == 0)
        def _():
            for p in range(len(steps)):
                @pl.when(e >= n_slot)
                def _():
                    load_w(e, p).wait()

                @pl.when(e + n_slot < local_exp)
                def _():
                    load_w(e + n_slot, p).start()
        return carry

    lax.fori_loop(0, local_exp, expert, 0)


def combine_kernel(z_ref, pm_hbm, wd_hbm, bd_hbm, x_hbm, out_ref,
                   bd_ref, x_ref, pm, wb, bias, yb, part, in0, in1, in2,
                   psem, lsem, wsem, s0, s1, s2, r0, r1, r2):
    local_exp, rows_all, d_ff = z_ref.shape
    n_src = 8
    cap = rows_all // n_src
    tok, d_model = x_hbm.shape
    n_col = d_model // COLS
    half = COLS // 2
    me = lax.axis_index('ep')
    barrier = pltpu.get_barrier_semaphore()
    for r in (1, 2, 4):
        pl.semaphore_signal(barrier, inc=1, device_id={'ep': flip(me, r)}, device_id_type=MESH)

    few = local_exp // 2

    def load_w(c, g):
        slot = lax.rem(c, 2)
        cols = pl.ds(pl.multiple_of(c * COLS, COLS), COLS)
        group = pl.ds(g * few, few)
        return pltpu.make_async_copy(wd_hbm.at[group, :, cols], wb.at[slot, group], wsem.at[slot, g])

    load_w(0, 0).start()
    load_w(0, 1).start()
    pload = pltpu.make_async_copy(pm_hbm, pm, psem)
    pload.start()
    bload = pltpu.make_async_copy(bd_hbm, bd_ref, lsem.at[0])
    xload = pltpu.make_async_copy(x_hbm, x_ref, lsem.at[1])
    bload.start()
    xload.start()
    bload.wait()
    bias[...] = bd_ref[...].astype(F32)

    def to_mate(c):
        return remote(part.at[c, 1], in0.at[c], s0.at[c], r0.at[c], flip(me, 1))

    def to_first(c, h):
        return remote(part.at[c, 0, h, pl.ds(2, 2)], in1.at[c, h], s1.at[c, h], r1.at[c, h], flip(me, 2 + 2 * h))

    def to_second(c, h):
        return remote(part.at[c, 0, h, 1], in2.at[c, h], s2.at[c, h], r2.at[c, h], flip(me, 4 - 2 * h))

    def merge_mate(c):
        to_mate(c).wait_recv()
        for js in ((2, 3), (0, 1)):
            for h in range(2):
                for j in js:
                    part[c, 0, h, j] = part[c, 0, h, j] + in0[c, h, j]
                if js[0] == 2:
                    to_first(c, h).start()

    def merge_first(c):
        for h in range(2):
            to_first(c, h).wait_recv()
            for j in (1, 0):
                part[c, 0, h, j] = part[c, 0, h, j] + in1[c, h, j]
            to_second(c, h).start()

    def finish(c):
        for h in range(2):
            to_second(c, h).wait_recv()
            cols = pl.ds(pl.multiple_of(c * COLS + h * half, half), half)
            out_ref[:, cols] = (x_ref[:, cols].astype(F32) + (part[c, 0, h, 0] + in2[c, h])).astype(BF16)

    def step(c, carry):
        slot = lax.rem(c, 2)
        cols = pl.ds(pl.multiple_of(c * COLS, COLS), COLS)

        @pl.when(c + 1 < n_col)
        def _():
            load_w(c + 1, 0).start()
            load_w(c + 1, 1).start()

        for g in range(2):
            load_w(c, g).wait()
            if g == 1:
                @pl.when(c == 0)
                def _():
                    pload.wait()
                    xload.wait()
                    pl.semaphore_wait(barrier, 3)

                @pl.when(c >= 1)
                def _():
                    merge_mate(c - 1)

            for e in range(g * few, (g + 1) * few):
                y = jnp.dot(z_ref[e], wb[slot, e], preferred_element_type=F32) + bias[e:e + 1, cols]
                y = y.astype(BF16)
                for s in range(n_src):
                    yb[s, e * cap:(e + 1) * cap, :] = y[s * cap:(s + 1) * cap, :]

        for core in (1, 0):
            for q in range(4):
                src = flip(me, 2 * q + core)
                sums = jnp.dot(pm[src], yb[src], preferred_element_type=F32)
                sums = (sums[2 * tok:] + sums[tok:2 * tok]) + sums[:tok]
                for h in range(2):
                    j = q if h == 1 or q in (0, 3) else 3 - q
                    part[c, core, h, j] = sums[:, h * half:(h + 1) * half]
            if core == 1:
                to_mate(c).start()

        @pl.when(c >= 2)
        def _():
            merge_first(c - 2)

        @pl.when(c >= 4)
        def _():
            finish(c - 4)
        return carry

    lax.fori_loop(0, n_col, step, 0)
    merge_mate(n_col - 1)
    for c in range(n_col - 2, n_col):
        merge_first(c)
    for c in range(n_col - 4, n_col):
        finish(c)
    for c in range(n_col):
        to_mate(c).wait_send()
        for h in range(2):
            to_first(c, h).wait_send()
            to_second(c, h).wait_send()


def solution(mesh):
    n_group = mesh.shape['ep']
    assert n_group == 8
    rows_spec = P(('dp', 'ep'), None)

    def local_block(x_in, expert_ids, norm_weight, router_w, router_b, w_gate_up, b_gate_up, w_down, b_down):
        tok, d_model = x_in.shape
        top_k = expert_ids.shape[1]
        local_exp, _, width = w_gate_up.shape
        d_ff = w_down.shape[1]
        experts = local_exp * n_group
        cap = CAPACITY_FACTOR * top_k * tok // experts
        rows_all = n_group * cap
        hbm = pl.BlockSpec(memory_space=pl.ANY)
        vmem = pl.BlockSpec(memory_space=pltpu.VMEM)
        smem = pl.BlockSpec(memory_space=pltpu.SMEM)
        dma = pltpu.SemaphoreType.DMA
        in_hbm = functools.partial(pltpu.with_memory_space_constraint, memory_space=pltpu.HBM)
        pinned = functools.partial(pltpu.with_memory_space_constraint, memory_space=pltpu.VMEM)
        xs, w_first, pm, counts = pl.pallas_call(
            functools.partial(dispatch_kernel, top_k, local_exp, cap),
            out_shape=(pltpu.VMEM((local_exp, n_group, cap, d_model), BF16),
                       pltpu.VMEM((N_RING, d_model, width), BF16),
                       pltpu.HBM((n_group, 3 * tok, local_exp * cap), BF16),
                       pltpu.HBM((local_exp, 128), jnp.int32)),
            in_specs=[hbm] * 6,
            out_specs=(vmem, vmem, hbm, hbm),
            scratch_shapes=[
                pltpu.VMEM((d_model,), BF16), pltpu.VMEM((experts, d_model), BF16), pltpu.VMEM((1, experts), BF16), pltpu.VMEM((local_exp, 128), jnp.int32),
                pltpu.VMEM((8, tok, d_model), BF16), pltpu.VMEM((8, top_k, tok), jnp.int32), pltpu.VMEM((tok, d_model), BF16),
                pltpu.VMEM((8, 128), F32), pltpu.VMEM((1, d_model), F32), pltpu.VMEM((tok, tok), BF16),
                pltpu.VMEM((8, local_exp * cap, tok), BF16), pltpu.VMEM((local_exp * cap, tok), F32),
                pltpu.VMEM((experts, tok), F32), pltpu.VMEM((8, local_exp, tok), F32),
                pltpu.VMEM((2, 3 * tok, local_exp * cap), BF16),
                dma((5,)), dma((2,)), dma((14,)), dma((8, 2)), dma((8,)), dma((8,)), dma((8,)), dma((8,)), dma((N_RING,))],
            compiler_params=pltpu.CompilerParams(collective_id=0, has_side_effects=True, vmem_limit_bytes=10 * MIB),
            name='dispatch',
        )(*map(in_hbm, (x_in, expert_ids.T, norm_weight, router_w.T, router_b.reshape(1, experts), w_gate_up)))
        z, _ = pl.pallas_call(
            gate_up_kernel,
            out_shape=(pltpu.VMEM((local_exp, rows_all, d_ff), BF16), pltpu.VMEM((N_RING, d_model, width), BF16)),
            in_specs=[hbm, vmem, vmem, hbm, hbm],
            out_specs=(vmem, vmem),
            input_output_aliases={2: 1},
            scratch_shapes=[
                pltpu.VMEM((rows_all, d_model), BF16), pltpu.VMEM((rows_all, width), BF16),
                pltpu.VMEM((local_exp, width), BF16), pltpu.VMEM((local_exp, width), F32), pltpu.VMEM((256, 256), BF16),
                pltpu.SMEM((local_exp, 128), jnp.int32), pltpu.SMEM((local_exp, 2 * rows_all // BLK), jnp.int32), pltpu.SMEM((local_exp,), jnp.int32),
                dma((N_RING, -(-width // NSTEP))), dma((2,))],
            compiler_params=pltpu.CompilerParams(vmem_limit_bytes=10 * MIB),
            name='gate_up',
        )(counts, pinned(xs), pinned(w_first), w_gate_up, in_hbm(b_gate_up))
        n_col = d_model // COLS
        return pl.pallas_call(
            combine_kernel,
            out_shape=pltpu.VMEM((tok, d_model), BF16),
            in_specs=[vmem, hbm, hbm, hbm, hbm],
            out_specs=vmem,
            scratch_shapes=[
                pltpu.VMEM((local_exp, d_model), BF16), pltpu.VMEM((tok, d_model), BF16),
                pltpu.VMEM((n_group, 3 * tok, local_exp * cap), BF16),
                pltpu.VMEM((2, local_exp, d_ff, COLS), BF16), pltpu.VMEM((local_exp, d_model), F32),
                pltpu.VMEM((n_group, local_exp * cap, COLS), BF16), pltpu.VMEM((n_col, 2, 2, 4, tok, COLS // 2), F32),
                pltpu.VMEM((n_col, 2, 4, tok, COLS // 2), F32), pltpu.VMEM((n_col, 2, 2, tok, COLS // 2), F32),
                pltpu.VMEM((n_col, 2, tok, COLS // 2), F32),
                dma, dma((2,)), dma((2, 2)), dma((n_col,)), dma((n_col, 2)), dma((n_col, 2)), dma((n_col,)), dma((n_col, 2)), dma((n_col, 2))],
            compiler_params=pltpu.CompilerParams(collective_id=1, has_side_effects=True, vmem_limit_bytes=55 * MIB),
            name='combine',
        )(pinned(z), in_hbm(pm), w_down, in_hbm(b_down), in_hbm(x_in))

    return jax.shard_map(local_block, mesh=mesh, in_specs=(rows_spec, rows_spec, P(), P(), P(), P('ep', None, None), P('ep', None), P('ep', None, None), P('ep', None)), out_specs=rows_spec, check_vma=False)
```

```python
import functools

import jax
import jax.numpy as jnp
from jax import lax
from jax.experimental import pallas as pl
from jax.experimental.pallas import tpu as pltpu
from jax.sharding import PartitionSpec as P

CAPACITY_FACTOR = 4
EPSILON = 1e-5
LIMIT = 7.0
ALPHA = 1.702
LOWEST = -3.3895313892515355e38
BLK = 16
COLS = 256
MESH = pl.DeviceIdType.MESH
F32 = jnp.float32
BF16 = jnp.bfloat16
MIB = 1024 * 1024
N_RING = 3
NSTEP = 1536


def flip(me, role):
    core = lax.rem(lax.rem(me, 2) + lax.rem(role, 2), 2)
    x = lax.rem(lax.rem(lax.div(me, 2), 2) + lax.rem(lax.div(role, 2), 2), 2)
    y = lax.rem(lax.div(me, 4) + lax.div(role, 4), 2)
    return y * 4 + x * 2 + core


def remote(src, dst, send, recv, device):
    return pltpu.make_async_remote_copy(src_ref=src, dst_ref=dst, send_sem=send, recv_sem=recv, device_id={'ep': device}, device_id_type=MESH)


def dispatch_kernel(top_k, local_exp, cap, x_hbm, ids_hbm, g_hbm, wr_hbm, br_hbm, wgu_hbm, xs_ref, wpre_ref, pm_hbm, cnt_hbm,
                    g_ref, wr_ref, br_ref, cnt_ref, xb, idb, hb, brp, gain, tri, oh, pt, probs, prb, pstage,
                    lsem, psem, ssem, rsem, isend, irecv, gsend, grecv, wsem):
    tok, d_model = x_hbm.shape
    experts = wr_ref.shape[0]
    half = tok // 2
    me = lax.axis_index('ep')
    load_x = pltpu.make_async_copy(x_hbm, xb.at[0], lsem.at[0])
    load_ids = pltpu.make_async_copy(ids_hbm, idb.at[0], lsem.at[1])
    load_x.start()
    load_ids.start()
    small = [pltpu.make_async_copy(a, b, lsem.at[k + 2]) for k, (a, b) in enumerate([(g_hbm, g_ref), (wr_hbm, wr_ref), (br_hbm, br_ref)])]
    for c in small:
        c.start()
    barrier = pltpu.get_barrier_semaphore()
    for r in range(1, 8):
        pl.semaphore_signal(barrier, inc=1, device_id={'ep': flip(me, r)}, device_id_type=MESH)
    load_x.wait()
    load_ids.wait()
    pl.semaphore_wait(barrier, 7)

    def piece(src_role, h, dst_role, to_role, k):
        rows = pl.ds(h * half, half)
        return remote(xb.at[src_role, rows], xb.at[dst_role, rows], ssem.at[k], rsem.at[dst_role, h], flip(me, to_role))

    def landed(role, h):
        piece(role, h, role, 1, 0).wait_recv()

    sends = [(0, 0, 2, 2), (0, 1, 4, 4), (0, 0, 1, 1), (0, 1, 1, 1), (0, 1, 2, 2), (0, 0, 4, 4)]
    relays = [(2, 0, 6, 4), (2, 0, 3, 1), (4, 1, 6, 2), (4, 1, 5, 1), (2, 1, 3, 1), (4, 0, 5, 1)]
    last = [(6, 0, 7, 1), (6, 1, 7, 1)]
    everything = sends + relays + last

    def go(k):
        piece(*everything[k], k).start()

    ids_out = [remote(idb.at[0], idb.at[r], isend.at[r], irecv.at[r], flip(me, r)) for r in range(1, 8)]
    for c in ids_out:
        c.start()
    for k in range(4):
        go(k)
    fetch = [pltpu.make_async_copy(wgu_hbm.at[e], wpre_ref.at[e], wsem.at[e]) for e in range(wpre_ref.shape[0])]
    for c in fetch:
        c.start()
    for c in small:
        c.wait()
    brp[...] = jnp.zeros_like(brp)
    brp[0:1, :experts] = br_ref[...].astype(F32)
    bias = jnp.transpose(jnp.broadcast_to(brp[0:1, :], (tok, tok)))[:experts]
    gain[...] = g_ref[...].astype(F32).reshape(gain.shape)
    tri[...] = (lax.broadcasted_iota(jnp.int32, (tok, tok), 0) < lax.broadcasted_iota(jnp.int32, (tok, tok), 1)).astype(F32).astype(BF16)
    cnt_ref[...] = jnp.zeros_like(cnt_ref)

    def normed(i):
        def norm(j, c):
            rows = pl.ds(pl.multiple_of(j * 64, 64), 64)
            xf = xb[i, rows, :].astype(F32)
            inv = lax.rsqrt(jnp.mean(xf * xf, axis=-1, keepdims=True) + EPSILON)
            hb[rows, :] = (xf * inv * gain[...]).astype(BF16)
            return c

        lax.fori_loop(0, tok // 64, norm, 0)

    normed(0)
    logits = lax.dot_general(wr_ref[...], hb[...], (((1,), (1,)), ((), ())), preferred_element_type=F32) + bias
    expert_no = lax.broadcasted_iota(jnp.int32, (experts, tok), 0)
    chosen = jnp.zeros((experts, tok), F32)
    for k in range(top_k):
        chosen = jnp.where(expert_no == idb[0, k:k + 1, :], 1.0, chosen)
    picked = jnp.where(chosen > 0, logits, -jnp.inf)
    ex = jnp.exp(picked - jnp.max(picked, axis=0, keepdims=True))
    probs[...] = ex / jnp.sum(ex, axis=0, keepdims=True)

    def block(device):
        return probs.at[pl.ds(pl.multiple_of(device * local_exp, local_exp), local_exp)]

    gates_out = [remote(block(flip(me, r)), prb.at[r], gsend.at[r], grecv.at[r], flip(me, r)) for r in range(1, 8)]
    for c in gates_out:
        c.start()
    go(4)
    go(5)
    prb[0] = probs[pl.ds(pl.multiple_of(me * local_exp, local_exp), local_exp), :]

    def seat(i, carry):
        @pl.when(i >= 1)
        def _():
            remote(idb.at[i], idb.at[i], isend.at[0], irecv.at[i], flip(me, 1)).wait_recv()

        src = flip(me, i)
        ids = idb[i]
        number = me * local_exp + lax.broadcasted_iota(jnp.int32, (local_exp, tok), 0)
        held = jnp.zeros((local_exp, tok), F32)
        for k in range(top_k):
            held = jnp.where(number == ids[k:k + 1, :], 1.0, held)
        rank = jnp.dot(held.astype(BF16), tri[...], preferred_element_type=F32)
        count = jnp.sum(held, axis=1, keepdims=True)
        lane = lax.broadcasted_iota(jnp.int32, cnt_ref.shape, 1)
        cnt_ref[...] = jnp.where(lane == src, count.astype(jnp.int32), cnt_ref[...])
        rank = jnp.where(held > 0, rank, -1.0)
        place = lax.broadcasted_iota(jnp.int32, (cap, tok), 0).astype(F32)
        for e in range(local_exp):
            oh[i, e * cap:(e + 1) * cap, :] = jnp.where(rank[e:e + 1, :] == place, 1.0, 0.0).astype(BF16)
        return carry

    lax.fori_loop(0, 8, seat, 0)
    landed(2, 0)
    go(6)
    go(7)
    landed(4, 1)
    go(8)
    go(9)

    def weigh(i, carry):
        @pl.when(i >= 1)
        def _():
            remote(prb.at[i], prb.at[i], gsend.at[0], grecv.at[i], flip(me, 1)).wait_recv()

        slot = lax.rem(i, 2)
        out_p = pltpu.make_async_copy(pstage.at[slot], pm_hbm.at[flip(me, i)], psem.at[slot])
        p_loc = prb[i]
        for e in range(local_exp):
            hit = oh[i, e * cap:(e + 1) * cap, :].astype(F32) > 0
            pt[e * cap:(e + 1) * cap, :] = jnp.where(hit, p_loc[e:e + 1, :], 0.0)

        @pl.when(i >= 2)
        def _():
            out_p.wait()

        for b in range(local_exp * cap // tok):
            p = jnp.transpose(pt[b * tok:(b + 1) * tok, :])
            for part in range(3):
                low = p.astype(BF16)
                pstage[slot, part * tok:(part + 1) * tok, b * tok:(b + 1) * tok] = low
                p = p - low.astype(F32)
        out_p.start()
        return carry

    lax.fori_loop(0, 8, weigh, 0)
    save_cnt = pltpu.make_async_copy(cnt_ref, cnt_hbm, lsem.at[0])
    save_cnt.start()

    def gather(i, carry):
        @pl.when(i == 1)
        def _():
            landed(1, 0)
            landed(1, 1)

        @pl.when(i == 2)
        def _():
            landed(2, 1)
            go(10)
            landed(4, 0)
            go(11)

        @pl.when(i == 3)
        def _():
            landed(3, 0)
            landed(3, 1)

        @pl.when(i == 5)
        def _():
            landed(5, 0)
            landed(5, 1)

        @pl.when(i == 6)
        def _():
            landed(6, 0)
            go(12)
            landed(6, 1)
            go(13)

        @pl.when(i == 7)
        def _():
            landed(7, 0)
            landed(7, 1)

        normed(i)
        src = flip(me, i)
        for n in range(0, d_model, 512):
            rows = jnp.dot(oh[i], hb[:, n:n + 512], preferred_element_type=F32).astype(BF16)
            for e in range(local_exp):
                xs_ref[e, src, :, n:n + 512] = rows[e * cap:(e + 1) * cap, :]
        return carry

    lax.fori_loop(0, 8, gather, 0)
    save_cnt.wait()
    for slot in range(2):
        pltpu.make_async_copy(pstage.at[slot], pm_hbm.at[me], psem.at[slot]).wait()
    for c in fetch:
        c.wait()
    for c in ids_out + gates_out:
        c.wait_send()
    for k in range(len(everything)):
        piece(*everything[k], k).wait_send()


def gate_up_kernel(cnt_hbm, xs_ref, wpre_ref, wgu_hbm, bgu_hbm, z_ref, wb, xc, uc, braw, bias, perm, cnt, blk, total, wsem, sem):
    local_exp, n_src, cap, d_model = xs_ref.shape
    width = wgu_hbm.shape[2]
    per_src = cap // BLK
    n_slot = wb.shape[0]

    steps = [(n0, min(NSTEP, width - n0)) for n0 in range(0, width, NSTEP)]

    def load_w(e, p):
        slot = lax.rem(e, n_slot)
        cols = pl.ds(*steps[p])
        return pltpu.make_async_copy(wgu_hbm.at[e, :, cols], wb.at[slot, :, cols], wsem.at[slot, p])

    load_cnt = pltpu.make_async_copy(cnt_hbm, cnt, sem.at[0])
    load_bias = pltpu.make_async_copy(bgu_hbm, braw, sem.at[1])
    load_cnt.start()
    load_bias.start()
    row = lax.broadcasted_iota(jnp.int32, perm.shape, 0)
    col = lax.broadcasted_iota(jnp.int32, perm.shape, 1)
    source = jnp.where(col < 128, 2 * col, 2 * col - 255)
    perm[...] = jnp.where(row == source, 1.0, 0.0).astype(BF16)

    def clear(e, carry):
        z_ref[e] = jnp.zeros(z_ref.shape[1:], BF16)
        return carry

    lax.fori_loop(0, local_exp, clear, 0)
    load_cnt.wait()

    def listed(e, carry):
        n = jnp.int32(0)
        prev = jnp.int32(0)
        for s in range(n_src):
            k = lax.div(cnt[e, s] + (BLK - 1), BLK)
            for b in range(per_src):
                prev = jnp.where(b < k, s * per_src + b, prev)
                blk[e, n + b] = prev
            n = n + k
        for j in range(n_src * per_src):
            blk[e, n + j] = prev
        total[e] = n
        return carry

    lax.fori_loop(0, local_exp, listed, 0)
    load_bias.wait()
    bias[...] = braw[...].astype(F32)

    def expert(e, carry):
        slot = lax.rem(e, n_slot)
        def run(rows):
            n = rows // BLK
            for j in range(n):
                b = blk[e, j]
                first = pl.multiple_of(lax.rem(b, per_src) * BLK, BLK)
                xc[j * BLK:(j + 1) * BLK, :] = xs_ref[e, lax.div(b, per_src), pl.ds(first, BLK), :]
            for p, (n0, w) in enumerate(steps):
                @pl.when(e >= n_slot)
                def _():
                    load_w(e, p).wait()

                u = jnp.dot(xc[0:rows, :], wb[slot, :, n0:n0 + w], preferred_element_type=F32) + bias[pl.ds(e, 1), n0:n0 + w]
                uc[0:rows, n0:n0 + w] = jnp.minimum(jnp.maximum(u, LOWEST), LIMIT).astype(BF16)

                @pl.when(e + n_slot < local_exp)
                def _():
                    load_w(e + n_slot, p).start()

            for m in range(0, width, 256):
                v = jnp.dot(uc[0:rows, m:m + 256], perm[...], preferred_element_type=F32)
                gate = v[:, :128]
                linear = jnp.maximum(v[:, 128:], -LIMIT)
                z = gate * lax.logistic(ALPHA * gate) * (linear + 1.0)
                z = z.astype(BF16)
                for j in range(n):
                    z_ref[e, pl.ds(pl.multiple_of(blk[e, j] * BLK, BLK), BLK), m // 2:m // 2 + 128] = z[j * BLK:(j + 1) * BLK, :]

        n = total[e]

        @pl.when(jnp.logical_and(n > 0, n <= 8))
        def _():
            run(128)

        @pl.when(jnp.logical_and(n > 8, n <= 16))
        def _():
            run(256)

        @pl.when(n > 16)
        def _():
            run(384)

        @pl.when(n == 0)
        def _():
            for p in range(len(steps)):
                @pl.when(e >= n_slot)
                def _():
                    load_w(e, p).wait()

                @pl.when(e + n_slot < local_exp)
                def _():
                    load_w(e + n_slot, p).start()
        return carry

    lax.fori_loop(0, local_exp, expert, 0)


def combine_kernel(z_ref, pm_hbm, wd_hbm, bd_hbm, x_hbm, out_ref,
                   bd_ref, x_ref, pm, wb, bias, yb, part, in0, in1, in2,
                   psem, lsem, wsem, s0, s1, s2, r0, r1, r2):
    local_exp, rows_all, d_ff = z_ref.shape
    n_src = 8
    cap = rows_all // n_src
    tok, d_model = x_hbm.shape
    n_col = d_model // COLS
    half = COLS // 2
    me = lax.axis_index('ep')
    barrier = pltpu.get_barrier_semaphore()
    for r in (1, 2, 4):
        pl.semaphore_signal(barrier, inc=1, device_id={'ep': flip(me, r)}, device_id_type=MESH)

    few = local_exp // 2

    def load_w(c, g):
        slot = lax.rem(c, 2)
        cols = pl.ds(pl.multiple_of(c * COLS, COLS), COLS)
        group = pl.ds(g * few, few)
        return pltpu.make_async_copy(wd_hbm.at[group, :, cols], wb.at[slot, group], wsem.at[slot, g])

    load_w(0, 0).start()
    load_w(0, 1).start()
    pload = pltpu.make_async_copy(pm_hbm, pm, psem)
    pload.start()
    bload = pltpu.make_async_copy(bd_hbm, bd_ref, lsem.at[0])
    xload = pltpu.make_async_copy(x_hbm, x_ref, lsem.at[1])
    bload.start()
    xload.start()
    bload.wait()
    bias[...] = bd_ref[...].astype(F32)

    def to_mate(c):
        return remote(part.at[c, 1], in0.at[c], s0.at[c], r0.at[c], flip(me, 1))

    def to_first(c, h):
        return remote(part.at[c, 0, h, pl.ds(2, 2)], in1.at[c, h], s1.at[c, h], r1.at[c, h], flip(me, 2 + 2 * h))

    def to_second(c, h):
        return remote(part.at[c, 0, h, 1], in2.at[c, h], s2.at[c, h], r2.at[c, h], flip(me, 4 - 2 * h))

    def merge_mate(c):
        to_mate(c).wait_recv()
        for js in ((2, 3), (0, 1)):
            for h in range(2):
                for j in js:
                    part[c, 0, h, j] = part[c, 0, h, j] + in0[c, h, j]
                if js[0] == 2:
                    to_first(c, h).start()

    def merge_first(c):
        for h in range(2):
            to_first(c, h).wait_recv()
            for j in (1, 0):
                part[c, 0, h, j] = part[c, 0, h, j] + in1[c, h, j]
            to_second(c, h).start()

    def finish(c):
        for h in range(2):
            to_second(c, h).wait_recv()
            cols = pl.ds(pl.multiple_of(c * COLS + h * half, half), half)
            out_ref[:, cols] = (x_ref[:, cols].astype(F32) + (part[c, 0, h, 0] + in2[c, h])).astype(BF16)

    def step(c, carry):
        slot = lax.rem(c, 2)
        cols = pl.ds(pl.multiple_of(c * COLS, COLS), COLS)

        @pl.when(c + 1 < n_col)
        def _():
            load_w(c + 1, 0).start()
            load_w(c + 1, 1).start()

        for g in range(2):
            load_w(c, g).wait()
            if g == 1:
                @pl.when(c == 0)
                def _():
                    pload.wait()
                    xload.wait()
                    pl.semaphore_wait(barrier, 3)

                @pl.when(c >= 1)
                def _():
                    merge_mate(c - 1)

                @pl.when(c >= 3)
                def _():
                    merge_first(c - 3)
                    pl.when(c >= 5)(lambda: finish(c - 5))

            for e in range(g * few, (g + 1) * few):
                y = jnp.dot(z_ref[e], wb[slot, e], preferred_element_type=F32) + bias[e:e + 1, cols]
                y = y.astype(BF16)
                for s in range(n_src):
                    yb[s, e * cap:(e + 1) * cap, :] = y[s * cap:(s + 1) * cap, :]

        for core in (1, 0):
            for q in range(4):
                src = flip(me, 2 * q + core)
                sums = jnp.dot(pm[src], yb[src], preferred_element_type=F32)
                sums = (sums[2 * tok:] + sums[tok:2 * tok]) + sums[:tok]
                for h in range(2):
                    j = q if h == 1 or q in (0, 3) else 3 - q
                    part[c, core, h, j] = sums[:, h * half:(h + 1) * half]
            if core == 1:
                to_mate(c).start()

        return carry

    lax.fori_loop(0, n_col, step, 0)
    merge_mate(n_col - 1)
    for c in range(n_col - 3, n_col):
        merge_first(c)
    for c in range(n_col - 5, n_col):
        finish(c)
    for c in range(n_col):
        to_mate(c).wait_send()
        for h in range(2):
            to_first(c, h).wait_send()
            to_second(c, h).wait_send()


def solution(mesh):
    n_group = mesh.shape['ep']
    assert n_group == 8
    rows_spec = P(('dp', 'ep'), None)

    def local_block(x_in, expert_ids, norm_weight, router_w, router_b, w_gate_up, b_gate_up, w_down, b_down):
        tok, d_model = x_in.shape
        top_k = expert_ids.shape[1]
        local_exp, _, width = w_gate_up.shape
        d_ff = w_down.shape[1]
        experts = local_exp * n_group
        cap = CAPACITY_FACTOR * top_k * tok // experts
        rows_all = n_group * cap
        hbm = pl.BlockSpec(memory_space=pl.ANY)
        vmem = pl.BlockSpec(memory_space=pltpu.VMEM)
        smem = pl.BlockSpec(memory_space=pltpu.SMEM)
        dma = pltpu.SemaphoreType.DMA
        in_hbm = functools.partial(pltpu.with_memory_space_constraint, memory_space=pltpu.HBM)
        pinned = functools.partial(pltpu.with_memory_space_constraint, memory_space=pltpu.VMEM)
        xs, w_first, pm, counts = pl.pallas_call(
            functools.partial(dispatch_kernel, top_k, local_exp, cap),
            out_shape=(pltpu.VMEM((local_exp, n_group, cap, d_model), BF16),
                       pltpu.VMEM((N_RING, d_model, width), BF16),
                       pltpu.HBM((n_group, 3 * tok, local_exp * cap), BF16),
                       pltpu.HBM((local_exp, 128), jnp.int32)),
            in_specs=[hbm] * 6,
            out_specs=(vmem, vmem, hbm, hbm),
            scratch_shapes=[
                pltpu.VMEM((d_model,), BF16), pltpu.VMEM((experts, d_model), BF16), pltpu.VMEM((1, experts), BF16), pltpu.VMEM((local_exp, 128), jnp.int32),
                pltpu.VMEM((8, tok, d_model), BF16), pltpu.VMEM((8, top_k, tok), jnp.int32), pltpu.VMEM((tok, d_model), BF16),
                pltpu.VMEM((8, 128), F32), pltpu.VMEM((1, d_model), F32), pltpu.VMEM((tok, tok), BF16),
                pltpu.VMEM((8, local_exp * cap, tok), BF16), pltpu.VMEM((local_exp * cap, tok), F32),
                pltpu.VMEM((experts, tok), F32), pltpu.VMEM((8, local_exp, tok), F32),
                pltpu.VMEM((2, 3 * tok, local_exp * cap), BF16),
                dma((5,)), dma((2,)), dma((14,)), dma((8, 2)), dma((8,)), dma((8,)), dma((8,)), dma((8,)), dma((N_RING,))],
            compiler_params=pltpu.CompilerParams(collective_id=0, has_side_effects=True, vmem_limit_bytes=10 * MIB),
            name='dispatch',
        )(*map(in_hbm, (x_in, expert_ids.T, norm_weight, router_w.T, router_b.reshape(1, experts), w_gate_up)))
        z, _ = pl.pallas_call(
            gate_up_kernel,
            out_shape=(pltpu.VMEM((local_exp, rows_all, d_ff), BF16), pltpu.VMEM((N_RING, d_model, width), BF16)),
            in_specs=[hbm, vmem, vmem, hbm, hbm],
            out_specs=(vmem, vmem),
            input_output_aliases={2: 1},
            scratch_shapes=[
                pltpu.VMEM((rows_all, d_model), BF16), pltpu.VMEM((rows_all, width), BF16),
                pltpu.VMEM((local_exp, width), BF16), pltpu.VMEM((local_exp, width), F32), pltpu.VMEM((256, 256), BF16),
                pltpu.SMEM((local_exp, 128), jnp.int32), pltpu.SMEM((local_exp, 2 * rows_all // BLK), jnp.int32), pltpu.SMEM((local_exp,), jnp.int32),
                dma((N_RING, -(-width // NSTEP))), dma((2,))],
            compiler_params=pltpu.CompilerParams(vmem_limit_bytes=10 * MIB),
            name='gate_up',
        )(counts, pinned(xs), pinned(w_first), w_gate_up, in_hbm(b_gate_up))
        n_col = d_model // COLS
        return pl.pallas_call(
            combine_kernel,
            out_shape=pltpu.VMEM((tok, d_model), BF16),
            in_specs=[vmem, hbm, hbm, hbm, hbm],
            out_specs=vmem,
            scratch_shapes=[
                pltpu.VMEM((local_exp, d_model), BF16), pltpu.VMEM((tok, d_model), BF16),
                pltpu.VMEM((n_group, 3 * tok, local_exp * cap), BF16),
                pltpu.VMEM((2, local_exp, d_ff, COLS), BF16), pltpu.VMEM((local_exp, d_model), F32),
                pltpu.VMEM((n_group, local_exp * cap, COLS), BF16), pltpu.VMEM((n_col, 2, 2, 4, tok, COLS // 2), F32),
                pltpu.VMEM((n_col, 2, 4, tok, COLS // 2), F32), pltpu.VMEM((n_col, 2, 2, tok, COLS // 2), F32),
                pltpu.VMEM((n_col, 2, tok, COLS // 2), F32),
                dma, dma((2,)), dma((2, 2)), dma((n_col,)), dma((n_col, 2)), dma((n_col, 2)), dma((n_col,)), dma((n_col, 2)), dma((n_col, 2))],
            compiler_params=pltpu.CompilerParams(collective_id=1, has_side_effects=True, vmem_limit_bytes=55 * MIB),
            name='combine',
        )(pinned(z), in_hbm(pm), w_down, in_hbm(b_down), in_hbm(x_in))

    return jax.shard_map(local_block, mesh=mesh, in_specs=(rows_spec, rows_spec, P(), P(), P(), P('ep', None, None), P('ep', None), P('ep', None, None), P('ep', None)), out_specs=rows_spec, check_vma=False)
```
